256 devices in a mesh: rows: 32 (over y, x, core), grp: 8 (over z).
Axes of the slice: x: 4, y: 4, z: 8, core: 2. Of those that a mesh axis runs over, the one named last changes fastest.
Arguments:
- matrix: bfloat16 [131072, 2048], P(('rows', 'grp')), may hold values from -0.0625 to 0.0625
- right_side: bfloat16 [131072, 128], P(('rows', 'grp')), may hold values from -6 to 6
- precond: bfloat16 [2048, 2048], replicated, may hold values from -1 to 3
- row_counts: int32 [256], P(('rows', 'grp')), may hold values from 64 to 512, as said below
Outputs:
- solution: float32 [2048, 128], P(None, 'grp')
- coeffs: float32 [2048, 128], P(None, 'grp')
- rel_residual: float32 [128], P('grp')
The draws below stay inside these ranges and needn't reach their ends.
Inputs may be any that keep to these rules, and one draw needn't show every extreme that they name: Device d holds A's rows in its first row_counts[d] slots of 512; some device is full in every draw.
All inputs are finite; a program needn't handle non-finite values.
Results may differ from the reference program's by a relative error of at most 0.0128.
Values may be sent and summed in bfloat16 or wider, within the bound.
A program may use at most 64 MiB of HBM per device.

```python
import math
import jax
import jax.numpy as jnp
from jax import lax

D = 2048
K = 128
ITERS = 3
R_DEV = 512
NDEV = 256
ROWS = 131072


def draw_row_counts(key, part):
    first, second = jax.random.split(key)
    base = jax.random.randint(first, (NDEV,), R_DEV // 8, R_DEV // 2 + 1, dtype=jnp.int32)
    fullest = jax.random.randint(second, (), 0, NDEV, dtype=jnp.int32)
    return jnp.where(jnp.arange(NDEV, dtype=jnp.int32) == fullest, R_DEV, base).astype(jnp.int32)


def draw_precond(key, part):
    first, second = jax.random.split(key)
    scales = jnp.exp(jax.random.uniform(first, (D,), minval=math.log(0.25), maxval=math.log(2.0)))
    noise = jax.random.normal(second, (D, D))
    return (jnp.diag(scales) + 0.5 * noise / math.sqrt(D)).astype(jnp.bfloat16)


def strengthened(values, stream_key, source, target, blocks, factor):
    def block_of(dim):
        return (jnp.arange(values.shape[dim]) // (values.shape[dim] // blocks)).reshape((-1,) + (1,) * (values.ndim - 1 - dim))

    near = jax.random.permutation(stream_key, blocks)[block_of(target)]
    second = (block_of(target) + blocks // 2) % blocks
    return jnp.where((block_of(source) == near) | (block_of(source) == second), factor * values, values)


def shard_levels(own_key, dims, shards, smallest, largest):
    def one(axis_at, blocks):
        steps = jax.random.uniform(jax.random.fold_in(jax.random.fold_in(own_key, 6), axis_at), (blocks,), jnp.float32, smallest / len(shards), largest / len(shards))
        return jnp.repeat(jnp.exp(steps), dims[axis_at] // blocks).reshape((-1,) + (1,) * (len(dims) - axis_at - 1))

    loudness = one(*shards[0])
    for cut in shards[1:]:
        loudness = loudness * one(*cut)
    return loudness


def normal_values(key, extent, width, reach, cuts=(), kind=jnp.bfloat16):
    loudness = shard_levels(key, extent, cuts, -0.22, 0.18) if cuts else 1.0
    values = jax.random.normal(key, extent, jnp.float32) * width * loudness
    return jnp.minimum(jnp.maximum(values, -reach), reach).astype(kind)


def noise_with(own_key, dims, width, reach, shards, heavy, kind=jnp.bfloat16):
    result = width * jax.random.normal(own_key, dims, jnp.float32)
    if shards:
        result = result * shard_levels(own_key, dims, shards, -0.22, 0.18)
    return jnp.clip(strengthened(result, jax.random.fold_in(own_key, 3), *heavy), -reach, reach).astype(kind)


def setup_inputs(seed: int = 0) -> dict:
    key_list = jax.random.split(jax.random.key(seed), 5)
    return {
        "matrix": noise_with(key_list[0], (ROWS, D), ROWS ** -0.5, 0.0625, ((0, 256),), (0, 1, 256, 6.0)),
        "right_side": normal_values(key_list[1], (ROWS, K), 1.0, 6.0, ((0, 256),)),
        "precond": draw_precond(jax.random.fold_in(key_list[4], 71), 0),
        "row_counts": draw_row_counts(jax.random.fold_in(key_list[4], 71), 0),
    }


floor_sq = 0.01

def pull_back(matrix, precond, residue):
    partial_value = lax.dot_general(matrix, residue.astype(jnp.bfloat16), (((0,), (0,)), ((), ())), preferred_element_type=jnp.float32)
    squares = lax.optimization_barrier(jnp.sum(residue * residue, axis=0, keepdims=True))
    u_norm = jnp.sqrt(squares + floor_sq)
    pulled = lax.dot_general(precond, (partial_value / u_norm).astype(jnp.bfloat16), (((0,), (0,)), ((), ())), preferred_element_type=jnp.float32)
    return (u_norm, pulled)

def reference(matrix, right_side, precond, row_counts):
    total_rows = matrix.shape[0]
    position = jnp.arange(total_rows, dtype=jnp.int32)
    owner = (position // R_DEV).astype(jnp.int32)
    live_rows = (position % R_DEV < row_counts[owner]).astype(jnp.float32)[:, None]
    residue = live_rows * right_side.astype(jnp.float32)
    u_norm, pulled = pull_back(matrix, precond, residue)
    v_norm = jnp.sqrt(lax.optimization_barrier(jnp.sum(pulled * pulled, axis=0, keepdims=True)) + floor_sq)
    right_vec = pulled / v_norm
    left_vec = residue / u_norm
    phi_bar = u_norm
    rho_bar = v_norm
    search = right_vec
    coeffs = jnp.zeros(right_vec.shape, jnp.float32)
    start_norm = u_norm
    for turn_index in range(ITERS):
        pushed = jnp.dot(precond, right_vec.astype(jnp.bfloat16), preferred_element_type=jnp.float32).astype(jnp.bfloat16)
        residue = live_rows * (jnp.dot(matrix, pushed, preferred_element_type=jnp.float32) - v_norm * left_vec)
        u_norm, pulled = pull_back(matrix, precond, residue)
        raw_vec = pulled - u_norm * right_vec
        next_norm = jnp.sqrt(lax.optimization_barrier(jnp.sum(raw_vec * raw_vec, axis=0, keepdims=True)) + floor_sq)
        next_vec = raw_vec / next_norm
        left_vec = residue / u_norm
        radius = jnp.sqrt(rho_bar * rho_bar + u_norm * u_norm)
        cosine = rho_bar / radius
        sine_part = u_norm / radius
        coupling = sine_part * next_norm
        rho_bar = -cosine * next_norm
        phi_step = cosine * phi_bar
        phi_bar = sine_part * phi_bar
        coeffs = coeffs + phi_step / radius * search
        search = next_vec - coupling / radius * search
        right_vec = next_vec
        v_norm = next_norm
    solution = jnp.dot(precond, coeffs.astype(jnp.bfloat16), preferred_element_type=jnp.float32)
    return (solution, coeffs, (phi_bar / start_norm)[0])
```

```python
import functools

import jax
import jax.numpy as jnp
from jax import lax
from jax.experimental import pallas as pl
from jax.experimental.pallas import tpu as pltpu
from jax.sharding import PartitionSpec as P

ITERS = 3
FLOOR_SQ = 0.01
MESH = pl.DeviceIdType.MESH
SIDE = 4
CHIPS = SIDE * SIDE
LANES = 128
TILE = 256

NT = (((1,), (1,)), ((), ()))


def dot(a, b):
    return jnp.dot(a, b, preferred_element_type=jnp.float32)


def dot_nt(a, b):
    return lax.dot_general(a, b, NT, preferred_element_type=jnp.float32)


def reach(step):
    return min(step, SIDE - step)


OFFSETS = sorted(
    ((dy, dx) for dy in range(SIDE) for dx in range(SIDE) if dy or dx),
    key=lambda o: -(reach(o[0]) + reach(o[1])),
)


def wide(column, count):
    return jnp.concatenate([column] * count, axis=1)


def kernel(
    planes,
    count_ref, a_hbm, b_hbm, n_hbm,
    sol_ref, coef_ref, ratio_ref,
    a, b, n, rv, vb, pushed, pref, pb, q, part, partb, crecv, xsend, xrecv, zbuf,
    csq, xsq, zsq, search, coeffs, rho, phi, start, ucol, vcol,
    load_sem, cs_sem, cr_sem, xs_sem, xr_sem, zs_sem, zr_sem, gs_sem, gr_sem, fs_sem, fr_sem,
    csqs_sem, csqr_sem, xsqs_sem, xsqr_sem, zsqs_sem, zsqr_sem,
):
    columns, width = rv.shape
    rows = a.shape[0]
    half = columns // 2
    own_cols = columns // planes
    tiles = width // TILE
    per_tile = TILE // LANES

    r = lax.axis_index("rows")
    z = lax.axis_index("grp")
    core = lax.rem(r, 2)
    chip = lax.div(r, 2)
    x = lax.rem(chip, SIDE)
    y = lax.div(chip, SIDE)

    def chip_at(dy, dx):
        return lax.rem(y + dy, SIDE) * SIDE + lax.rem(x + dx, SIDE)

    plane_chips = [chip_at(dy, dx) for dy, dx in OFFSETS]
    other_planes = [lax.rem(z + k, planes) for k in sorted(range(1, planes), key=lambda k: -min(k, planes - k))]
    partner = {"rows": chip * 2 + (1 - core), "grp": z}

    def on_chip(c):
        return {"rows": c * 2 + core, "grp": z}

    def on_plane(k):
        return {"rows": r, "grp": k}

    def remote(src, dst, send, recv, device):
        return pltpu.make_async_remote_copy(
            src_ref=src, dst_ref=dst, send_sem=send, recv_sem=recv, device_id=device, device_id_type=MESH
        )

    barrier = pltpu.get_barrier_semaphore()
    partners = [partner] + [on_chip(c) for c in plane_chips] + [on_plane(k) for k in other_planes]
    for device in partners:
        pl.semaphore_signal(barrier, inc=1, device_id=device, device_id_type=MESH)

    load_b = pltpu.make_async_copy(b_hbm, b, load_sem.at[0])
    load_a = pltpu.make_async_copy(a_hbm, a, load_sem.at[1])
    load_n = pltpu.make_async_copy(n_hbm, n, load_sem.at[2])
    load_b.start()
    load_a.start()
    load_n.start()

    live = (lax.broadcasted_iota(jnp.int32, (columns, rows), 1) < count_ref[0]).astype(jnp.float32)
    ones = jnp.ones((8, rows), jnp.bfloat16)

    def keep_squares(residue):
        square = residue * residue
        high = square.astype(jnp.bfloat16)
        low = (square - high.astype(jnp.float32)).astype(jnp.bfloat16)
        total = dot_nt(ones, high) + dot_nt(ones, low)
        csq[0] = total[0:1]

    def keep_residue(residue):
        pref[...] = residue
        pb[...] = residue.astype(jnp.bfloat16)
        keep_squares(residue)

    rv[...] = jnp.zeros_like(rv)
    search[...] = jnp.zeros_like(search)
    coeffs[...] = jnp.zeros_like(coeffs)
    rho[...] = jnp.zeros_like(rho)
    phi[...] = jnp.zeros_like(phi)
    start[...] = jnp.zeros_like(start)

    load_b.wait()
    keep_residue(live * jnp.transpose(b[...].astype(jnp.float32)))
    load_a.wait()
    pl.semaphore_wait(barrier, len(partners))

    def core_copy(j):
        theirs = pl.ds((1 - core) * half, half)
        block = pl.ds(j * per_tile, per_tile)
        return remote(partb.at[block, theirs], crecv.at[block], cs_sem.at[j], cr_sem.at[j], partner)

    core_sq = remote(csq.at[0], csq.at[1], csqs_sem, csqr_sem, partner)

    def plane_copy(c):
        return remote(xsend.at[c], xrecv.at[chip], xs_sem.at[c], xr_sem.at[chip], on_chip(c))

    def plane_arrival(c):
        return remote(xsend.at[c], xrecv.at[c], xs_sem.at[c], xr_sem.at[c], on_chip(c))

    def plane_sq(c):
        return remote(xsq.at[chip], xsq.at[chip], xsqs_sem.at[c], xsqr_sem.at[chip], on_chip(c))

    def plane_sq_arrival(c):
        return remote(xsq.at[c], xsq.at[c], xsqs_sem.at[c], xsqr_sem.at[c], on_chip(c))

    def depth_copy(par, k):
        return remote(zbuf.at[par, z], zbuf.at[par, z], zs_sem.at[par, k], zr_sem.at[par, z], on_plane(k))

    def depth_arrival(par, k):
        return remote(zbuf.at[par, k], zbuf.at[par, k], zs_sem.at[par, k], zr_sem.at[par, k], on_plane(k))

    def depth_sq(par, k):
        return remote(zsq.at[par, z], zsq.at[par, z], zsqs_sem.at[par, k], zsqr_sem.at[par, z], on_plane(k))

    def depth_sq_arrival(par, k):
        return remote(zsq.at[par, k], zsq.at[par, k], zsqs_sem.at[par, k], zsqr_sem.at[par, k], on_plane(k))

    def piece(c, h):
        return q.at[pl.ds(pl.multiple_of(h * half, half), half), pl.ds(pl.multiple_of(c * LANES, LANES), LANES)]

    def gather_copy(c):
        return remote(piece(chip, core), piece(chip, core), gs_sem.at[c], gr_sem.at[chip], on_chip(c))

    def gather_arrival(c):
        return remote(piece(c, core), piece(c, core), gs_sem.at[c], gr_sem.at[c], on_chip(c))

    def forward_copy(c):
        return remote(piece(c, core), piece(c, core), fs_sem.at[c], fr_sem.at[c], partner)

    def forward_arrival(c):
        return remote(piece(c, 1 - core), piece(c, 1 - core), fs_sem.at[c], fr_sem.at[c], partner)

    def squares_plane():
        core_sq.wait_recv()
        xsq[chip] = csq[0] + csq[1]
        for c in plane_chips:
            plane_sq(c).start()

    def squares_depth(par):
        for c in plane_chips:
            plane_sq_arrival(c).wait_recv()
        total = xsq[0]
        for c in range(1, CHIPS):
            total = total + xsq[c]
        zsq[par, z] = total
        for k in other_planes:
            depth_sq(par, k).start()

    def squares_total(par):
        for k in other_planes:
            depth_sq_arrival(par, k).wait_recv()
        total = zsq[par, 0]
        for k in range(1, planes):
            total = total + zsq[par, k]
        spread = jnp.transpose(jnp.broadcast_to(total, (columns, columns)))
        ucol[...] = jnp.sqrt(spread + FLOOR_SQ)

    def squares_sent(par):
        core_sq.wait_send()
        for c in plane_chips:
            plane_sq(c).wait_send()
        for k in other_planes:
            depth_sq(par, k).wait_send()

    mine = pl.ds(pl.multiple_of(z * own_cols, own_cols), own_cols)

    def turn(i, carry):
        par = lax.rem(i, 2)

        core_sq.start()
        residue = pb[...]
        for j in range(tiles):
            product = dot(residue, a[:, j * TILE : (j + 1) * TILE])
            for s in range(per_tile):
                chunk = product[:, s * LANES : (s + 1) * LANES]
                part[j * per_tile + s] = chunk
                partb[j * per_tile + s] = chunk.astype(jnp.bfloat16)
            if j:
                core_copy(j - 1).start()
        core_copy(tiles - 1).start()

        @pl.when(i == 0)
        def _():
            load_n.wait()

        ours = pl.ds(pl.multiple_of(core * half, half), half)
        for j in range(tiles):
            core_copy(j).wait_recv()
        before = None
        for c in plane_chips:
            xsend[c] = (part[c, ours] + crecv[c].astype(jnp.float32)).astype(jnp.bfloat16)
            if before is not None:
                plane_copy(before).start()
            before = c
        own = part[chip, ours] + crecv[chip].astype(jnp.float32)
        plane_copy(before).start()
        squares_plane()
        for c in reversed(plane_chips):
            plane_arrival(c).wait_recv()
            own = own + xrecv[c].astype(jnp.float32)
        zbuf[par, z] = own.astype(jnp.bfloat16)
        squares_depth(par)
        for k in other_planes:
            depth_copy(par, k).start()

        squares_total(par)
        for k in reversed(other_planes):
            depth_arrival(par, k).wait_recv()
        total = zbuf[par, 0].astype(jnp.float32)
        for k in range(1, planes):
            total = total + zbuf[par, k].astype(jnp.float32)
        scaled = (total / ucol[ours]).astype(jnp.bfloat16)
        q[ours, pl.ds(pl.multiple_of(chip * LANES, LANES), LANES)] = scaled

        for c in plane_chips:
            gather_copy(c).start()
        forward_copy(chip).start()
        for c in reversed(plane_chips):
            gather_arrival(c).wait_recv()
            forward_copy(c).start()
        for j in range(tiles):
            core_copy(j).wait_send()
        for c in plane_chips:
            plane_copy(c).wait_send()
        for k in other_planes:
            depth_copy(par, k).wait_send()
        squares_sent(par)
        forward_arrival(chip).wait_recv()
        for c in reversed(plane_chips):
            forward_arrival(c).wait_recv()

        u = ucol[...]
        u_tile = wide(u, per_tile)
        gathered = q[...]
        squares = jnp.zeros((columns, LANES), jnp.float32)
        for j in range(tiles):
            at = slice(j * TILE, (j + 1) * TILE)
            raw = dot(gathered, n[:, at]) - u_tile * rv[:, at]
            rv[:, at] = raw
            for s in range(per_tile):
                block = raw[:, s * LANES : (s + 1) * LANES]
                squares = squares + block * block
        v = jnp.sqrt(jnp.sum(squares, axis=1, keepdims=True) + FLOOR_SQ)
        v = jnp.broadcast_to(v, (columns, LANES))
        vcol[...] = v
        v_tile = wide(v, per_tile)
        for j in range(tiles):
            at = slice(j * TILE, (j + 1) * TILE)
            unit = rv[:, at] / v_tile
            rv[:, at] = unit
            vb[:, at] = unit.astype(jnp.bfloat16)

        unit = vb[...]
        for j in range(tiles):
            at = slice(j * TILE, (j + 1) * TILE)
            pushed[:, at] = dot_nt(unit, n[at, :]).astype(jnp.bfloat16)
        front = pushed[...]
        image = jnp.concatenate(
            [dot_nt(front, a[j * TILE : (j + 1) * TILE, :]) for j in range(rows // TILE)], axis=1
        )
        keep_residue(live * (image - wide(v / u, rows // LANES) * pref[...]))

        u_own = ucol[mine]
        first = i == 0
        unit_own = rv[mine]
        v_own = vcol[mine]
        radius = jnp.sqrt(rho[...] * rho[...] + u_own * u_own)
        cosine = rho[...] / radius
        sine = u_own / radius
        coupling = sine * v_own
        phi_step = cosine * phi[...]
        coeffs[...] = coeffs[...] + wide(phi_step / radius, width // LANES) * search[...]
        search[...] = unit_own - wide(coupling / radius, width // LANES) * search[...]
        rho[...] = jnp.where(first, v_own, -cosine * v_own)
        phi[...] = jnp.where(first, u_own, sine * phi[...])
        start[...] = jnp.where(first, u_own, start[...])

        for c in plane_chips:
            gather_copy(c).wait_send()
            forward_copy(c).wait_send()
        forward_copy(chip).wait_send()
        return carry

    lax.fori_loop(0, ITERS, turn, 0)

    par = ITERS % 2
    core_sq.start()
    squares_plane()
    squares_depth(par)
    squares_total(par)
    squares_sent(par)
    u_own = ucol[mine]
    radius = jnp.sqrt(rho[...] * rho[...] + u_own * u_own)
    cosine = rho[...] / radius
    sine = u_own / radius
    result = coeffs[...] + wide(cosine * phi[...] / radius, width // LANES) * search[...]
    coef_ref[...] = result
    ratio_ref[...] = sine * phi[...] / start[...]
    narrow = result.astype(jnp.bfloat16)
    for j in range(tiles):
        at = slice(j * TILE, (j + 1) * TILE)
        sol_ref[:, at] = dot_nt(narrow, n[at, :])


def shards(planes, matrix, right_side, precond, row_counts):
    rows, width = matrix.shape
    columns = right_side.shape[1]
    own_cols = columns // planes
    half = columns // 2
    tiles = width // TILE
    vmem, dma = pltpu.VMEM, pltpu.SemaphoreType.DMA
    bf16, f32 = jnp.bfloat16, jnp.float32
    solution, coeffs, ratio = pl.pallas_call(
        functools.partial(kernel, planes),
        out_shape=(
            jax.ShapeDtypeStruct((own_cols, width), f32),
            jax.ShapeDtypeStruct((own_cols, width), f32),
            jax.ShapeDtypeStruct((own_cols, LANES), f32),
        ),
        in_specs=[pl.BlockSpec(memory_space=pltpu.SMEM)] + [pl.BlockSpec(memory_space=pl.ANY)] * 3,
        out_specs=(pl.BlockSpec(memory_space=vmem),) * 3,
        scratch_shapes=[
            vmem((rows, width), bf16),
            vmem((rows, columns), bf16),
            vmem((width, width), bf16),
            vmem((columns, width), f32),
            vmem((columns, width), bf16),
            vmem((columns, width), bf16),
            vmem((columns, rows), f32),
            vmem((columns, rows), bf16),
            vmem((columns, width), bf16),
            vmem((CHIPS, columns, LANES), f32),
            vmem((CHIPS, columns, LANES), bf16),
            vmem((CHIPS, half, LANES), bf16),
            vmem((CHIPS, half, LANES), bf16),
            vmem((CHIPS, half, LANES), bf16),
            vmem((2, planes, half, LANES), bf16),
            vmem((2, 1, columns), f32),
            vmem((CHIPS, 1, columns), f32),
            vmem((2, planes, 1, columns), f32),
            vmem((own_cols, width), f32),
            vmem((own_cols, width), f32),
            vmem((own_cols, LANES), f32),
            vmem((own_cols, LANES), f32),
            vmem((own_cols, LANES), f32),
            vmem((columns, LANES), f32),
            vmem((columns, LANES), f32),
            dma((3,)),
            dma((tiles,)), dma((tiles,)),
            dma((CHIPS,)), dma((CHIPS,)),
            dma((2, planes)), dma((2, planes)),
            dma((CHIPS,)), dma((CHIPS,)),
            dma((CHIPS,)), dma((CHIPS,)),
            dma, dma,
            dma((CHIPS,)), dma((CHIPS,)),
            dma((2, planes)), dma((2, planes)),
        ],
        compiler_params=pltpu.CompilerParams(
            collective_id=0, has_side_effects=True, vmem_limit_bytes=60 * 1024 * 1024
        ),
    )(row_counts, matrix, right_side, precond)
    return solution.T, coeffs.T, ratio[:, 0]


def solution(mesh):
    return jax.shard_map(
        functools.partial(shards, mesh.shape["grp"]),
        mesh=mesh,
        in_specs=(P(("rows", "grp"), None), P(("rows", "grp"), None), P(), P(("rows", "grp"))),
        out_specs=(P(None, "grp"), P(None, "grp"), P("grp")),
        check_vma=False,
    )
```

```python
import functools

import jax
import jax.numpy as jnp
from jax import lax
from jax.experimental import pallas as pl
from jax.experimental.pallas import tpu as pltpu
from jax.sharding import PartitionSpec as P

ITERS = 3
FLOOR_SQ = 0.01
MESH = pl.DeviceIdType.MESH
SIDE = 4
CHIPS = SIDE * SIDE
LANES = 128
TILE = 256
GROUP = SIDE * LANES

SEND_ROWS = (2, 1, 3, 0)
SEND_COLS = (2, 1, 3, 0)
TAKE_ROWS = (2, 1, 3, 0)

NT = (((1,), (1,)), ((), ()))


def dot(a, b):
    return jnp.dot(a, b, preferred_element_type=jnp.float32)


def dot_nt(a, b):
    return lax.dot_general(a, b, NT, preferred_element_type=jnp.float32)


def wide(column, count):
    return jnp.concatenate([column] * count, axis=1)


def halves(value):
    high = value.astype(jnp.bfloat16)
    return high, (value - high.astype(jnp.float32)).astype(jnp.bfloat16)


def kernel(
    planes,
    count_ref, a_hbm, b_hbm, n_hbm,
    sol_ref, coef_ref, ratio_ref,
    a, at, b, n, nt, rv, raw, vb, pushed, pref, pb, p0, q, part, partb, crecv, xsend, xrecv, ownrow, zbuf,
    live, csq, xsq, zsq, fsq, state, scalars, ucol, vcol,
    load_sem, cs_sem, cr_sem, ps_sem, pr_sem, ls_sem, lr_sem, as_sem, ar_sem,
    xs_sem, xr_sem, zs_sem, zr_sem, gs_sem, gr_sem,
    xsqs_sem, xsqr_sem, zsqs_sem, zsqr_sem, fsqs_sem, fsqr_sem, ts_sem, tr_sem, us_sem, ur_sem,
):
    half, width = rv.shape
    columns = 2 * half
    rows = b.shape[0]
    both = 2 * rows
    own_cols = columns // planes
    per_core = planes // 2

    r = lax.axis_index("rows")
    z = lax.axis_index("grp")
    core = lax.rem(r, 2)
    chip = lax.div(r, 2)
    x = lax.rem(chip, SIDE)
    y = lax.div(chip, SIDE)

    def row_at(dy):
        return lax.rem(y + dy, SIDE)

    def chip_at(dy, dx):
        return row_at(dy) * SIDE + lax.rem(x + dx, SIDE)

    offsets = [(dy, dx) for dy in SEND_ROWS for dx in SEND_COLS if dy or dx]
    plane_chips = [chip_at(dy, dx) for dy, dx in offsets]
    other_planes = [lax.rem(z + k, planes) for k in sorted(range(1, planes), key=lambda k: -min(k, planes - k))]
    partner = {"rows": chip * 2 + (1 - core), "grp": z}

    def on_chip(c):
        return {"rows": c * 2 + core, "grp": z}

    def on_plane(k, other=False):
        return {"rows": chip * 2 + (1 - core) if other else r, "grp": k}

    def remote(src, dst, send, recv, device):
        return pltpu.make_async_remote_copy(
            src_ref=src, dst_ref=dst, send_sem=send, recv_sem=recv, device_id=device, device_id_type=MESH
        )

    barrier = pltpu.get_barrier_semaphore()
    partners = (
        [partner]
        + [on_chip(c) for c in plane_chips]
        + [on_plane(k) for k in other_planes]
        + [on_plane(k, True) for k in other_planes]
    )
    for device in partners:
        pl.semaphore_signal(barrier, inc=1, device_id=device, device_id_type=MESH)

    load_b = pltpu.make_async_copy(b_hbm, b, load_sem.at[0])
    load_a = pltpu.make_async_copy(a_hbm, a.at[pl.ds(0, rows)], load_sem.at[1])
    load_n = pltpu.make_async_copy(n_hbm, n, load_sem.at[2])
    load_b.start()
    load_a.start()
    load_n.start()

    ours = pl.ds(pl.multiple_of(core * half, half), half)
    theirs = pl.ds(pl.multiple_of((1 - core) * half, half), half)
    ones = jnp.ones((8, both), jnp.bfloat16)

    core_copy = remote(partb.at[theirs], crecv, cs_sem, cr_sem, partner)
    residue_copy = remote(p0.at[theirs], p0.at[pl.ds(columns, half)], ps_sem, pr_sem, partner)
    live_copy = remote(live.at[0], live.at[1], ls_sem, lr_sem, partner)
    a_copy = remote(a.at[pl.ds(0, rows)], a.at[pl.ds(rows, rows)], as_sem, ar_sem, partner)
    state_copy = remote(state.at[core], state.at[core], ts_sem, tr_sem, partner)
    state_arrival = remote(state.at[1 - core], state.at[1 - core], ts_sem, tr_sem, partner)
    scalars_copy = remote(scalars.at[core], scalars.at[core], us_sem, ur_sem, partner)
    scalars_arrival = remote(scalars.at[1 - core], scalars.at[1 - core], us_sem, ur_sem, partner)

    def plane_copy(c):
        return remote(xsend.at[c], xrecv.at[chip], xs_sem.at[c], xr_sem.at[chip], on_chip(c))

    def plane_arrival(c):
        return remote(xsend.at[c], xrecv.at[c], xs_sem.at[c], xr_sem.at[c], on_chip(c))

    def plane_sq(c):
        return remote(xsq.at[chip], xsq.at[chip], xsqs_sem.at[c], xsqr_sem.at[chip], on_chip(c))

    def plane_sq_arrival(c):
        return remote(xsq.at[c], xsq.at[c], xsqs_sem.at[c], xsqr_sem.at[c], on_chip(c))

    def depth_copy(par, k):
        return remote(zbuf.at[par, z], zbuf.at[par, z], zs_sem.at[par, k], zr_sem.at[par, z], on_plane(k))

    def depth_arrival(par, k):
        return remote(zbuf.at[par, k], zbuf.at[par, k], zs_sem.at[par, k], zr_sem.at[par, k], on_plane(k))

    def depth_sq(par, k):
        return remote(zsq.at[par, z], zsq.at[par, z], zsqs_sem.at[par, k], zsqr_sem.at[par, z], on_plane(k))

    def depth_sq_arrival(par, k):
        return remote(zsq.at[par, k], zsq.at[par, k], zsqs_sem.at[par, k], zsqr_sem.at[par, k], on_plane(k))

    def last_sq(k, other):
        there = (1 - core) if other else core
        return remote(fsq.at[core, z], fsq.at[core, z], fsqs_sem.at[there, k], fsqr_sem.at[core, z], on_plane(k, other))

    def last_sq_arrival(h, k):
        return remote(fsq.at[h, k], fsq.at[h, k], fsqs_sem.at[h, k], fsqr_sem.at[h, k], partner)

    def piece(c):
        return q.at[:, pl.ds(pl.multiple_of(c * LANES, LANES), LANES)]

    def gather_copy(c):
        return remote(piece(chip), piece(chip), gs_sem.at[c], gr_sem.at[chip], on_chip(c))

    def gather_arrival(c):
        return remote(piece(c), piece(c), gs_sem.at[c], gr_sem.at[c], on_chip(c))

    def keep_squares():
        square = pref[...] * pref[...]
        blank = jnp.zeros_like(square)
        square = jnp.concatenate(
            [jnp.where(core == 0, square, blank), jnp.where(core == 0, blank, square)], axis=0
        )
        high, low = halves(square)
        total = dot_nt(ones, high) + dot_nt(ones, low)
        csq[...] = total[0:1]

    def squares_plane():
        xsq[chip] = csq[...]
        for c in plane_chips:
            plane_sq(c).start()

    def squares_of_plane():
        for c in plane_chips:
            plane_sq_arrival(c).wait_recv()
        total = xsq[0]
        for c in range(1, CHIPS):
            total = total + xsq[c]
        return total

    def keep_norm(total):
        spread = jnp.transpose(jnp.broadcast_to(total, (columns, columns)))
        ucol[...] = jnp.sqrt(spread + FLOOR_SQ)

    def send_group(value, dy):
        line = row_at(dy) * SIDE
        for s in range(SIDE):
            block = value[:, s * LANES : (s + 1) * LANES]
            xsend[line + s] = block.astype(jnp.bfloat16)
            if dy == 0:
                ownrow[s] = block
        for dx in SEND_COLS:
            if dy or dx:
                plane_copy(chip_at(dy, dx)).start()

    rv[...] = jnp.zeros_like(rv)
    state[...] = jnp.zeros_like(state)
    scalars[...] = jnp.zeros_like(scalars)
    shown = (lax.broadcasted_iota(jnp.int32, (1, rows), 1) < count_ref[0]).astype(jnp.float32)
    live[0] = shown
    load_b.wait()
    first_residue = shown * jnp.transpose(b[...].astype(jnp.float32))
    p0[pl.ds(0, columns)] = first_residue.astype(jnp.bfloat16)
    load_a.wait()

    start_residue = p0[pl.ds(0, columns)]
    for j in range(width // TILE):
        lanes = slice(j * TILE, (j + 1) * TILE)
        product = dot(start_residue, a[pl.ds(0, rows), lanes])
        part[:, lanes] = product
        partb[:, lanes] = product.astype(jnp.bfloat16)
    pl.semaphore_wait(barrier, len(partners))
    core_copy.start()
    residue_copy.start()
    live_copy.start()
    a_copy.start()

    mine = pl.ds(pl.multiple_of(lax.rem(z, per_core) * own_cols, own_cols), own_cols)
    spread = width // LANES

    def turn(i, carry):
        par = lax.rem(i, 2)

        @pl.when(i == 0)
        def _():
            core_copy.wait_recv()
            for dy in SEND_ROWS:
                lanes = pl.ds(pl.multiple_of(row_at(dy) * GROUP, GROUP), GROUP)
                send_group(part[ours, lanes] + crecv[:, lanes].astype(jnp.float32), dy)
            residue_copy.wait_recv()
            pref[...] = jnp.concatenate([p0[ours], p0[pl.ds(columns, half)]], axis=1).astype(jnp.float32)
            keep_squares()

        @pl.when(i > 0)
        def _():
            residue = pb[...]
            for dy in SEND_ROWS:
                lanes = pl.ds(pl.multiple_of(row_at(dy) * GROUP, GROUP), GROUP)
                send_group(dot(residue, a[:, lanes]), dy)

        squares_plane()

        @pl.when(i == 0)
        def _():
            lines = lax.broadcasted_iota(jnp.int32, (TILE, TILE), 0)
            same = (lines == lax.broadcasted_iota(jnp.int32, (TILE, TILE), 1)).astype(jnp.bfloat16)
            load_n.wait()

            def flip_n(k, c):
                here = pl.ds(pl.multiple_of(k * TILE, TILE), TILE)
                for j in range(width // TILE):
                    lanes = slice(j * TILE, (j + 1) * TILE)
                    nt[lanes, here] = dot_nt(same, n[here, lanes]).astype(jnp.bfloat16)
                return c

            lax.fori_loop(0, width // TILE, flip_n, 0)

        own = ownrow[x]
        for c in plane_chips:
            plane_arrival(c).wait_recv()
            own = own + xrecv[c].astype(jnp.float32)
        zbuf[par, z] = own.astype(jnp.bfloat16)
        zsq[par, z] = squares_of_plane()
        for k in other_planes:
            depth_copy(par, k).start()
            depth_sq(par, k).start()

        @pl.when(i == 0)
        def _():
            lines = lax.broadcasted_iota(jnp.int32, (TILE, TILE), 0)
            same = (lines == lax.broadcasted_iota(jnp.int32, (TILE, TILE), 1)).astype(jnp.bfloat16)
            a_copy.wait_recv()
            live_copy.wait_recv()

            def flip_a(k, c):
                here = pl.ds(pl.multiple_of(k * TILE, TILE), TILE)
                for j in range(width // TILE):
                    lanes = slice(j * TILE, (j + 1) * TILE)
                    at[lanes, here] = dot_nt(same, a[here, lanes]).astype(jnp.bfloat16)
                return c

            lax.fori_loop(0, both // TILE, flip_a, 0)

        for k in other_planes:
            depth_sq_arrival(par, k).wait_recv()
        total = zsq[par, 0]
        for k in range(1, planes):
            total = total + zsq[par, k]
        keep_norm(total)
        u = ucol[ours]
        for k in other_planes:
            depth_arrival(par, k).wait_recv()
        total = zbuf[par, 0].astype(jnp.float32)
        for k in range(1, planes):
            total = total + zbuf[par, k].astype(jnp.float32)
        q[:, pl.ds(pl.multiple_of(chip * LANES, LANES), LANES)] = (total / u).astype(jnp.bfloat16)

        for c in plane_chips:
            gather_copy(c).start()
        u_tile = wide(u, TILE // LANES)
        squares = jnp.zeros((half, LANES), jnp.float32)
        for turn_at, dy in enumerate(TAKE_ROWS):
            for dx in SEND_COLS:
                if dy or dx:
                    gather_arrival(chip_at(dy, dx)).wait_recv()
            here = pl.ds(pl.multiple_of(row_at(dy) * GROUP, GROUP), GROUP)
            taken = q[:, here]
            for j in range(width // TILE):
                lanes = slice(j * TILE, (j + 1) * TILE)
                before = raw[:, lanes] if turn_at else -u_tile * rv[:, lanes]
                value = before + dot(taken, n[here, lanes])
                raw[:, lanes] = value
                if turn_at == SIDE - 1:
                    for s in range(TILE // LANES):
                        block = value[:, s * LANES : (s + 1) * LANES]
                        squares = squares + block * block
        v = jnp.sqrt(jnp.sum(squares, axis=1, keepdims=True) + FLOOR_SQ)
        v = jnp.broadcast_to(v, (half, LANES))
        vcol[...] = v
        inverse = wide(1.0 / v, TILE // LANES)
        for j in range(width // TILE):
            lanes = slice(j * TILE, (j + 1) * TILE)
            unit = raw[:, lanes] * inverse
            rv[:, lanes] = unit
            vb[:, lanes] = unit.astype(jnp.bfloat16)

        unit = vb[...]
        for j in range(width // TILE):
            lanes = slice(j * TILE, (j + 1) * TILE)
            pushed[:, lanes] = dot(unit, nt[:, lanes]).astype(jnp.bfloat16)
        front = pushed[...]
        back = wide(v / u, rows // LANES)
        for h in range(2):
            lanes = slice(h * rows, (h + 1) * rows)
            residue = live[h] * (dot(front, at[:, lanes]) - back * pref[:, lanes])
            pref[:, lanes] = residue
            pb[:, lanes] = residue.astype(jnp.bfloat16)

        for c in plane_chips:
            plane_copy(c).wait_send()
            plane_sq(c).wait_send()
        keep_squares()

        first = i == 0
        u_own = ucol[pl.ds(pl.multiple_of(core * half, half) + lax.rem(z, per_core) * own_cols, own_cols)]
        v_own = vcol[mine]
        rho, phi, start = (scalars[core, pl.ds(k * own_cols, own_cols)] for k in range(3))
        search = state[core, pl.ds(own_cols, own_cols)]
        radius = jnp.sqrt(rho * rho + u_own * u_own)
        cosine = rho / radius
        sine = u_own / radius
        state[core, pl.ds(0, own_cols)] = (
            state[core, pl.ds(0, own_cols)] + wide(cosine * phi / radius, spread) * search
        )
        state[core, pl.ds(own_cols, own_cols)] = rv[mine] - wide(sine * v_own / radius, spread) * search
        scalars[core, pl.ds(0, own_cols)] = jnp.where(first, v_own, -cosine * v_own)
        scalars[core, pl.ds(own_cols, own_cols)] = jnp.where(first, u_own, sine * phi)
        scalars[core, pl.ds(2 * own_cols, own_cols)] = jnp.where(first, u_own, start)

        for k in other_planes:
            depth_copy(par, k).wait_send()
            depth_sq(par, k).wait_send()
        for c in plane_chips:
            gather_copy(c).wait_send()
        return carry

    lax.fori_loop(0, ITERS, turn, 0)

    squares_plane()
    state_copy.start()
    scalars_copy.start()
    fsq[core, z] = squares_of_plane()
    last_core = remote(fsq.at[core, z], fsq.at[core, z], fsqs_sem.at[1 - core, z], fsqr_sem.at[core, z], partner)
    for k in other_planes:
        last_sq(k, False).start()
        last_sq(k, True).start()
    last_core.start()

    holder = lax.div(z, per_core)
    state_arrival.wait_recv()
    scalars_arrival.wait_recv()
    high, low = halves(state[holder])
    stacked = jnp.concatenate([high, low], axis=0)
    for j in range(width // TILE):
        lanes = slice(j * TILE, (j + 1) * TILE)
        product = dot(stacked, nt[:, lanes])
        raw[pl.ds(0, 2 * own_cols), lanes] = product[: 2 * own_cols] + product[2 * own_cols :]

    last_sq_arrival(1 - core, z).wait_recv()
    for k in other_planes:
        last_sq_arrival(0, k).wait_recv()
        last_sq_arrival(1, k).wait_recv()
    total = fsq[0, 0]
    for h in range(2):
        for k in range(planes):
            if h or k:
                total = total + fsq[h, k]
    keep_norm(total)
    u_own = ucol[pl.ds(pl.multiple_of(z * own_cols, own_cols), own_cols)]
    rho, phi, start = (scalars[holder, pl.ds(k * own_cols, own_cols)] for k in range(3))
    radius = jnp.sqrt(rho * rho + u_own * u_own)
    cosine = rho / radius
    sine = u_own / radius
    step = wide(cosine * phi / radius, spread)
    coef_ref[...] = state[holder, pl.ds(0, own_cols)] + step * state[holder, pl.ds(own_cols, own_cols)]
    sol_ref[...] = raw[pl.ds(0, own_cols)] + step * raw[pl.ds(own_cols, own_cols)]
    ratio_ref[...] = sine * phi / start

    for copy in (core_copy, residue_copy, live_copy, a_copy, state_copy, scalars_copy, last_core):
        copy.wait_send()
    for c in plane_chips:
        plane_sq(c).wait_send()
    for k in other_planes:
        last_sq(k, False).wait_send()
        last_sq(k, True).wait_send()


def shards(planes, matrix, right_side, precond, row_counts):
    rows, width = matrix.shape
    columns = right_side.shape[1]
    own_cols = columns // planes
    half = columns // 2
    vmem, dma = pltpu.VMEM, pltpu.SemaphoreType.DMA
    bf16, f32 = jnp.bfloat16, jnp.float32
    solution, coeffs, ratio = pl.pallas_call(
        functools.partial(kernel, planes),
        out_shape=(
            jax.ShapeDtypeStruct((own_cols, width), f32),
            jax.ShapeDtypeStruct((own_cols, width), f32),
            jax.ShapeDtypeStruct((own_cols, LANES), f32),
        ),
        in_specs=[pl.BlockSpec(memory_space=pltpu.SMEM)] + [pl.BlockSpec(memory_space=pl.ANY)] * 3,
        out_specs=(pl.BlockSpec(memory_space=vmem),) * 3,
        scratch_shapes=[
            vmem((2 * rows, width), bf16),
            vmem((width, 2 * rows), bf16),
            vmem((rows, columns), bf16),
            vmem((width, width), bf16),
            vmem((width, width), bf16),
            vmem((half, width), f32),
            vmem((half, width), f32),
            vmem((half, width), bf16),
            vmem((half, width), bf16),
            vmem((half, 2 * rows), f32),
            vmem((half, 2 * rows), bf16),
            vmem((columns + half, rows), bf16),
            vmem((half, width), bf16),
            vmem((columns, width), f32),
            vmem((columns, width), bf16),
            vmem((half, width), bf16),
            vmem((CHIPS, half, LANES), bf16),
            vmem((CHIPS, half, LANES), bf16),
            vmem((SIDE, half, LANES), f32),
            vmem((2, planes, half, LANES), bf16),
            vmem((2, 1, rows), f32),
            vmem((1, columns), f32),
            vmem((CHIPS, 1, columns), f32),
            vmem((2, planes, 1, columns), f32),
            vmem((2, planes, 1, columns), f32),
            vmem((2, 2 * own_cols, width), f32),
            vmem((2, 3 * own_cols, LANES), f32),
            vmem((columns, LANES), f32),
            vmem((half, LANES), f32),
            dma((3,)),
            dma, dma, dma, dma, dma, dma, dma, dma,
            dma((CHIPS,)), dma((CHIPS,)),
            dma((2, planes)), dma((2, planes)),
            dma((CHIPS,)), dma((CHIPS,)),
            dma((CHIPS,)), dma((CHIPS,)),
            dma((2, planes)), dma((2, planes)),
            dma((2, planes)), dma((2, planes)),
            dma, dma, dma, dma,
        ],
        compiler_params=pltpu.CompilerParams(
            collective_id=0, has_side_effects=True, vmem_limit_bytes=60 * 1024 * 1024
        ),
    )(row_counts, matrix, right_side, precond)
    return solution.T, coeffs.T, ratio[:, 0]


def solution(mesh):
    return jax.shard_map(
        functools.partial(shards, mesh.shape["grp"]),
        mesh=mesh,
        in_specs=(P(("rows", "grp"), None), P(("rows", "grp"), None), P(), P(("rows", "grp"))),
        out_specs=(P(None, "grp"), P(None, "grp"), P("grp")),
        check_vma=False,
    )
```

```python
import functools

import jax
import jax.numpy as jnp
from jax import lax
from jax.experimental import pallas as pl
from jax.experimental.pallas import tpu as pltpu
from jax.sharding import PartitionSpec as P

ITERS = 3
FLOOR_SQ = 0.01
MESH = pl.DeviceIdType.MESH
SIDE = 4
CHIPS = SIDE * SIDE
LANES = 128
TILE = 256
GROUP = SIDE * LANES

SEND_ROWS = (2, 1, 3, 0)
SEND_COLS = (2, 1, 3, 0)
TAKE_ROWS = (2, 1, 3, 0)

NT = (((1,), (1,)), ((), ()))


def dot(a, b):
    return jnp.dot(a, b, preferred_element_type=jnp.float32)


def dot_nt(a, b):
    return lax.dot_general(a, b, NT, preferred_element_type=jnp.float32)


def wide(column, count):
    return jnp.concatenate([column] * count, axis=1)


def halves(value):
    high = value.astype(jnp.bfloat16)
    return high, (value - high.astype(jnp.float32)).astype(jnp.bfloat16)


def kernel(
    planes,
    count_ref, a_hbm, b_hbm, n_hbm,
    sol_ref, coef_ref, ratio_ref,
    a, at, b, n, nt, rv, raw, vb, pushed, pref, pb, p0, q, part, partb, crecv, xsend, xrecv, ownrow, zbuf,
    live, csq, xsq, zsq, fsq, state, scalars, ucol, vcol,
    load_sem, cs_sem, cr_sem, ps_sem, pr_sem, ls_sem, lr_sem, as_sem, ar_sem,
    xs_sem, xr_sem, zs_sem, zr_sem, gs_sem, gr_sem,
    xsqs_sem, xsqr_sem, zsqs_sem, zsqr_sem, fsqs_sem, fsqr_sem, ts_sem, tr_sem, us_sem, ur_sem,
):
    half, width = rv.shape
    columns = 2 * half
    rows = b.shape[0]
    both = 2 * rows
    own_cols = columns // planes
    per_core = planes // 2

    r = lax.axis_index("rows")
    z = lax.axis_index("grp")
    core = lax.rem(r, 2)
    chip = lax.div(r, 2)
    x = lax.rem(chip, SIDE)
    y = lax.div(chip, SIDE)

    def row_at(dy):
        return lax.rem(y + dy, SIDE)

    def chip_at(dy, dx):
        return row_at(dy) * SIDE + lax.rem(x + dx, SIDE)

    offsets = [(dy, dx) for dy in SEND_ROWS for dx in SEND_COLS if dy or dx]
    plane_chips = [chip_at(dy, dx) for dy, dx in offsets]
    other_planes = [lax.rem(z + k, planes) for k in sorted(range(1, planes), key=lambda k: -min(k, planes - k))]
    partner = {"rows": chip * 2 + (1 - core), "grp": z}

    def on_chip(c):
        return {"rows": c * 2 + core, "grp": z}

    def on_plane(k, other=False):
        return {"rows": chip * 2 + (1 - core) if other else r, "grp": k}

    def remote(src, dst, send, recv, device):
        return pltpu.make_async_remote_copy(
            src_ref=src, dst_ref=dst, send_sem=send, recv_sem=recv, device_id=device, device_id_type=MESH
        )

    barrier = pltpu.get_barrier_semaphore()
    partners = [on_plane(k, other) for k in other_planes for other in (False, True)]
    partners += [on_chip(c) for c in plane_chips] + [partner]
    for device in partners:
        pl.semaphore_signal(barrier, inc=1, device_id=device, device_id_type=MESH)

    load_b = pltpu.make_async_copy(b_hbm, b, load_sem.at[0])
    load_a = pltpu.make_async_copy(a_hbm, a.at[pl.ds(0, rows)], load_sem.at[1])
    load_n = pltpu.make_async_copy(n_hbm, n, load_sem.at[2])
    load_b.start()
    load_a.start()

    ours = pl.ds(pl.multiple_of(core * half, half), half)
    theirs = pl.ds(pl.multiple_of((1 - core) * half, half), half)
    ones = jnp.ones((8, both), jnp.bfloat16)

    core_copy = remote(partb.at[theirs], crecv, cs_sem, cr_sem, partner)
    residue_copy = remote(p0.at[theirs], p0.at[pl.ds(columns, half)], ps_sem, pr_sem, partner)
    live_copy = remote(live.at[0], live.at[1], ls_sem, lr_sem, partner)
    a_copy = remote(a.at[pl.ds(0, rows)], a.at[pl.ds(rows, rows)], as_sem, ar_sem, partner)
    state_copy = remote(state.at[core], state.at[core], ts_sem, tr_sem, partner)
    state_arrival = remote(state.at[1 - core], state.at[1 - core], ts_sem, tr_sem, partner)
    scalars_copy = remote(scalars.at[core], scalars.at[core], us_sem, ur_sem, partner)
    scalars_arrival = remote(scalars.at[1 - core], scalars.at[1 - core], us_sem, ur_sem, partner)

    def plane_copy(c):
        return remote(xsend.at[c], xrecv.at[chip], xs_sem.at[c], xr_sem.at[chip], on_chip(c))

    def plane_arrival(c):
        return remote(xsend.at[c], xrecv.at[c], xs_sem.at[c], xr_sem.at[c], on_chip(c))

    def plane_sq(c):
        return remote(xsq.at[chip], xsq.at[chip], xsqs_sem.at[c], xsqr_sem.at[chip], on_chip(c))

    def plane_sq_arrival(c):
        return remote(xsq.at[c], xsq.at[c], xsqs_sem.at[c], xsqr_sem.at[c], on_chip(c))

    def depth_copy(par, k):
        return remote(zbuf.at[par, z], zbuf.at[par, z], zs_sem.at[par, k], zr_sem.at[par, z], on_plane(k))

    def depth_arrival(par, k):
        return remote(zbuf.at[par, k], zbuf.at[par, k], zs_sem.at[par, k], zr_sem.at[par, k], on_plane(k))

    def depth_sq(par, k):
        return remote(zsq.at[par, z], zsq.at[par, z], zsqs_sem.at[par, k], zsqr_sem.at[par, z], on_plane(k))

    def depth_sq_arrival(par, k):
        return remote(zsq.at[par, k], zsq.at[par, k], zsqs_sem.at[par, k], zsqr_sem.at[par, k], on_plane(k))

    def last_sq(k, other):
        there = (1 - core) if other else core
        return remote(fsq.at[core, z], fsq.at[core, z], fsqs_sem.at[there, k], fsqr_sem.at[core, z], on_plane(k, other))

    def last_sq_arrival(h, k):
        return remote(fsq.at[h, k], fsq.at[h, k], fsqs_sem.at[h, k], fsqr_sem.at[h, k], partner)

    def piece(c):
        return q.at[:, pl.ds(pl.multiple_of(c * LANES, LANES), LANES)]

    def gather_copy(c):
        return remote(piece(chip), piece(chip), gs_sem.at[c], gr_sem.at[chip], on_chip(c))

    def gather_arrival(c):
        return remote(piece(c), piece(c), gs_sem.at[c], gr_sem.at[c], on_chip(c))

    def keep_squares():
        square = pref[...] * pref[...]
        blank = jnp.zeros_like(square)
        square = jnp.concatenate(
            [jnp.where(core == 0, square, blank), jnp.where(core == 0, blank, square)], axis=0
        )
        high, low = halves(square)
        total = dot_nt(ones, high) + dot_nt(ones, low)
        csq[...] = total[0:1]

    def squares_plane():
        xsq[chip] = csq[...]
        for c in plane_chips:
            plane_sq(c).start()

    def squares_of_plane():
        for c in plane_chips:
            plane_sq_arrival(c).wait_recv()
        total = xsq[0]
        for c in range(1, CHIPS):
            total = total + xsq[c]
        return total

    def keep_norm(total):
        spread = jnp.transpose(jnp.broadcast_to(total, (columns, columns)))
        ucol[...] = jnp.sqrt(spread + FLOOR_SQ)

    def send_group(value, dy):
        line = row_at(dy) * SIDE
        for s in range(SIDE):
            block = value[:, s * LANES : (s + 1) * LANES]
            xsend[line + s] = block.astype(jnp.bfloat16)
            if dy == 0:
                ownrow[s] = block
        for dx in SEND_COLS:
            if dy or dx:
                plane_copy(chip_at(dy, dx)).start()

    rv[...] = jnp.zeros_like(rv)
    state[...] = jnp.zeros_like(state)
    scalars[...] = jnp.zeros_like(scalars)
    shown = (lax.broadcasted_iota(jnp.int32, (1, rows), 1) < count_ref[0]).astype(jnp.float32)
    live[0] = shown
    load_b.wait()
    first_residue = shown * jnp.transpose(b[...].astype(jnp.float32))
    p0[pl.ds(0, columns)] = first_residue.astype(jnp.bfloat16)
    load_a.wait()
    load_n.start()

    start_residue = p0[pl.ds(0, columns)]
    for j in range(width // TILE):
        lanes = slice(j * TILE, (j + 1) * TILE)
        product = dot(start_residue, a[pl.ds(0, rows), lanes])
        part[:, lanes] = product
        partb[:, lanes] = product.astype(jnp.bfloat16)
    pl.semaphore_wait(barrier, len(partners))
    core_copy.start()
    residue_copy.start()
    live_copy.start()
    a_copy.start()

    mine = pl.ds(pl.multiple_of(lax.rem(z, per_core) * own_cols, own_cols), own_cols)
    spread = width // LANES

    def recur(first):
        u_own = ucol[pl.ds(pl.multiple_of(core * half, half) + lax.rem(z, per_core) * own_cols, own_cols)]
        v_own = vcol[mine]
        rho, phi, start = (scalars[core, pl.ds(k * own_cols, own_cols)] for k in range(3))
        search = state[core, pl.ds(own_cols, own_cols)]
        radius = jnp.sqrt(rho * rho + u_own * u_own)
        cosine = rho / radius
        sine = u_own / radius
        state[core, pl.ds(0, own_cols)] = (
            state[core, pl.ds(0, own_cols)] + wide(cosine * phi / radius, spread) * search
        )
        state[core, pl.ds(own_cols, own_cols)] = rv[mine] - wide(sine * v_own / radius, spread) * search
        scalars[core, pl.ds(0, own_cols)] = jnp.where(first, v_own, -cosine * v_own)
        scalars[core, pl.ds(own_cols, own_cols)] = jnp.where(first, u_own, sine * phi)
        scalars[core, pl.ds(2 * own_cols, own_cols)] = jnp.where(first, u_own, start)

    def turn(i, carry):
        par = lax.rem(i, 2)

        @pl.when(i == 0)
        def _():
            core_copy.wait_recv()
            for dy in SEND_ROWS:
                lanes = pl.ds(pl.multiple_of(row_at(dy) * GROUP, GROUP), GROUP)
                send_group(part[ours, lanes] + crecv[:, lanes].astype(jnp.float32), dy)
            residue_copy.wait_recv()
            pref[...] = jnp.concatenate([p0[ours], p0[pl.ds(columns, half)]], axis=1).astype(jnp.float32)

        @pl.when(i > 0)
        def _():
            residue = pb[...]
            for dy in SEND_ROWS:
                lanes = pl.ds(pl.multiple_of(row_at(dy) * GROUP, GROUP), GROUP)
                send_group(dot(residue, a[:, lanes]), dy)

        keep_squares()
        squares_plane()

        @pl.when(i > 0)
        def _():
            recur(i == 1)

        @pl.when(i == 0)
        def _():
            lines = lax.broadcasted_iota(jnp.int32, (TILE, TILE), 0)
            same = (lines == lax.broadcasted_iota(jnp.int32, (TILE, TILE), 1)).astype(jnp.bfloat16)
            load_n.wait()

            def flip_n(k, c):
                here = pl.ds(pl.multiple_of(k * TILE, TILE), TILE)
                for j in range(width // TILE):
                    lanes = slice(j * TILE, (j + 1) * TILE)
                    nt[lanes, here] = dot_nt(same, n[here, lanes]).astype(jnp.bfloat16)
                return c

            lax.fori_loop(0, width // TILE, flip_n, 0)

        own = ownrow[x]
        for c in plane_chips:
            plane_arrival(c).wait_recv()
            own = own + xrecv[c].astype(jnp.float32)
        zbuf[par, z] = own.astype(jnp.bfloat16)
        zsq[par, z] = squares_of_plane()
        for k in other_planes:
            depth_copy(par, k).start()
            depth_sq(par, k).start()

        @pl.when(i == 0)
        def _():
            lines = lax.broadcasted_iota(jnp.int32, (TILE, TILE), 0)
            same = (lines == lax.broadcasted_iota(jnp.int32, (TILE, TILE), 1)).astype(jnp.bfloat16)
            a_copy.wait_recv()
            live_copy.wait_recv()

            def flip_a(k, c):
                here = pl.ds(pl.multiple_of(k * TILE, TILE), TILE)
                for j in range(width // TILE):
                    lanes = slice(j * TILE, (j + 1) * TILE)
                    at[lanes, here] = dot_nt(same, a[here, lanes]).astype(jnp.bfloat16)
                return c

            lax.fori_loop(0, both // TILE, flip_a, 0)

        for k in other_planes:
            depth_sq_arrival(par, k).wait_recv()
        total = zsq[par, 0]
        for k in range(1, planes):
            total = total + zsq[par, k]
        keep_norm(total)
        u = ucol[ours]
        for k in other_planes:
            depth_arrival(par, k).wait_recv()
        total = zbuf[par, 0].astype(jnp.float32)
        for k in range(1, planes):
            total = total + zbuf[par, k].astype(jnp.float32)
        q[:, pl.ds(pl.multiple_of(chip * LANES, LANES), LANES)] = (total / u).astype(jnp.bfloat16)

        for c in plane_chips:
            gather_copy(c).start()
        u_tile = wide(u, TILE // LANES)
        squares = jnp.zeros((half, LANES), jnp.float32)
        for turn_at, dy in enumerate(TAKE_ROWS):
            for dx in SEND_COLS:
                if dy or dx:
                    gather_arrival(chip_at(dy, dx)).wait_recv()
            here = pl.ds(pl.multiple_of(row_at(dy) * GROUP, GROUP), GROUP)
            taken = q[:, here]
            for j in range(width // TILE):
                lanes = slice(j * TILE, (j + 1) * TILE)
                before = raw[:, lanes] if turn_at else -u_tile * rv[:, lanes]
                value = before + dot(taken, n[here, lanes])
                raw[:, lanes] = value
                if turn_at == SIDE - 1:
                    for s in range(TILE // LANES):
                        block = value[:, s * LANES : (s + 1) * LANES]
                        squares = squares + block * block
        v = jnp.sqrt(jnp.sum(squares, axis=1, keepdims=True) + FLOOR_SQ)
        v = jnp.broadcast_to(v, (half, LANES))
        vcol[...] = v
        inverse = wide(1.0 / v, TILE // LANES)
        for j in range(width // TILE):
            lanes = slice(j * TILE, (j + 1) * TILE)
            unit = raw[:, lanes] * inverse
            rv[:, lanes] = unit
            vb[:, lanes] = unit.astype(jnp.bfloat16)

        unit = vb[...]
        for j in range(width // TILE):
            lanes = slice(j * TILE, (j + 1) * TILE)
            pushed[:, lanes] = dot(unit, nt[:, lanes]).astype(jnp.bfloat16)
        front = pushed[...]
        back = wide(v / u, rows // LANES)
        for h in range(2):
            lanes = slice(h * rows, (h + 1) * rows)
            residue = live[h] * (dot(front, at[:, lanes]) - back * pref[:, lanes])
            pref[:, lanes] = residue
            pb[:, lanes] = residue.astype(jnp.bfloat16)

        for c in plane_chips:
            plane_copy(c).wait_send()
            plane_sq(c).wait_send()

        for k in other_planes:
            depth_copy(par, k).wait_send()
            depth_sq(par, k).wait_send()
        for c in plane_chips:
            gather_copy(c).wait_send()
        return carry

    lax.fori_loop(0, ITERS, turn, 0)

    keep_squares()
    squares_plane()
    recur(ITERS == 1)
    fsq[core, z] = squares_of_plane()
    last_core = remote(fsq.at[core, z], fsq.at[core, z], fsqs_sem.at[1 - core, z], fsqr_sem.at[core, z], partner)
    for k in other_planes:
        last_sq(k, False).start()
        last_sq(k, True).start()
    last_core.start()
    state_copy.start()
    scalars_copy.start()

    holder = lax.div(z, per_core)
    state_arrival.wait_recv()
    scalars_arrival.wait_recv()
    high, low = halves(state[holder])
    stacked = jnp.concatenate([high, low], axis=0)
    for j in range(width // TILE):
        lanes = slice(j * TILE, (j + 1) * TILE)
        product = dot(stacked, nt[:, lanes])
        raw[pl.ds(0, 2 * own_cols), lanes] = product[: 2 * own_cols] + product[2 * own_cols :]

    last_sq_arrival(1 - core, z).wait_recv()
    for k in other_planes:
        last_sq_arrival(0, k).wait_recv()
        last_sq_arrival(1, k).wait_recv()
    total = fsq[0, 0]
    for h in range(2):
        for k in range(planes):
            if h or k:
                total = total + fsq[h, k]
    keep_norm(total)
    u_own = ucol[pl.ds(pl.multiple_of(z * own_cols, own_cols), own_cols)]
    rho, phi, start = (scalars[holder, pl.ds(k * own_cols, own_cols)] for k in range(3))
    radius = jnp.sqrt(rho * rho + u_own * u_own)
    cosine = rho / radius
    sine = u_own / radius
    step = wide(cosine * phi / radius, spread)
    coef_ref[...] = state[holder, pl.ds(0, own_cols)] + step * state[holder, pl.ds(own_cols, own_cols)]
    sol_ref[...] = raw[pl.ds(0, own_cols)] + step * raw[pl.ds(own_cols, own_cols)]
    ratio_ref[...] = sine * phi / start

    for copy in (core_copy, residue_copy, live_copy, a_copy, state_copy, scalars_copy, last_core):
        copy.wait_send()
    for c in plane_chips:
        plane_sq(c).wait_send()
    for k in other_planes:
        last_sq(k, False).wait_send()
        last_sq(k, True).wait_send()


def finish(sol_in, coef_in, ratio_in, sol_ref, coef_ref, ratio_ref):
    sol_ref[...] = sol_in[...]
    coef_ref[...] = coef_in[...]
    ratio = ratio_in[...]
    square = jnp.concatenate([ratio] * (LANES // ratio.shape[0]), axis=0)
    ratio_ref[...] = jnp.transpose(square)[0:1, : ratio.shape[0]]


def shards(planes, matrix, right_side, precond, row_counts):
    rows, width = matrix.shape
    columns = right_side.shape[1]
    own_cols = columns // planes
    half = columns // 2
    vmem, dma = pltpu.VMEM, pltpu.SemaphoreType.DMA
    bf16, f32 = jnp.bfloat16, jnp.float32
    solution, coeffs, ratio = pl.pallas_call(
        functools.partial(kernel, planes),
        out_shape=(
            jax.ShapeDtypeStruct((own_cols, width), f32),
            jax.ShapeDtypeStruct((own_cols, width), f32),
            jax.ShapeDtypeStruct((own_cols, LANES), f32),
        ),
        in_specs=[pl.BlockSpec(memory_space=pltpu.SMEM)] + [pl.BlockSpec(memory_space=pl.ANY)] * 3,
        out_specs=(pl.BlockSpec(memory_space=vmem),) * 3,
        scratch_shapes=[
            vmem((2 * rows, width), bf16),
            vmem((width, 2 * rows), bf16),
            vmem((rows, columns), bf16),
            vmem((width, width), bf16),
            vmem((width, width), bf16),
            vmem((half, width), f32),
            vmem((half, width), f32),
            vmem((half, width), bf16),
            vmem((half, width), bf16),
            vmem((half, 2 * rows), f32),
            vmem((half, 2 * rows), bf16),
            vmem((columns + half, rows), bf16),
            vmem((half, width), bf16),
            vmem((columns, width), f32),
            vmem((columns, width), bf16),
            vmem((half, width), bf16),
            vmem((CHIPS, half, LANES), bf16),
            vmem((CHIPS, half, LANES), bf16),
            vmem((SIDE, half, LANES), f32),
            vmem((2, planes, half, LANES), bf16),
            vmem((2, 1, rows), f32),
            vmem((1, columns), f32),
            vmem((CHIPS, 1, columns), f32),
            vmem((2, planes, 1, columns), f32),
            vmem((2, planes, 1, columns), f32),
            vmem((2, 2 * own_cols, width), f32),
            vmem((2, 3 * own_cols, LANES), f32),
            vmem((columns, LANES), f32),
            vmem((half, LANES), f32),
            dma((3,)),
            dma, dma, dma, dma, dma, dma, dma, dma,
            dma((CHIPS,)), dma((CHIPS,)),
            dma((2, planes)), dma((2, planes)),
            dma((CHIPS,)), dma((CHIPS,)),
            dma((CHIPS,)), dma((CHIPS,)),
            dma((2, planes)), dma((2, planes)),
            dma((2, planes)), dma((2, planes)),
            dma, dma, dma, dma,
        ],
        compiler_params=pltpu.CompilerParams(
            collective_id=0, has_side_effects=True, vmem_limit_bytes=60 * 1024 * 1024
        ),
    )(row_counts, matrix, right_side, precond)
    solution, coeffs, ratio = pl.pallas_call(
        finish,
        out_shape=(
            jax.ShapeDtypeStruct((own_cols, width), f32),
            jax.ShapeDtypeStruct((own_cols, width), f32),
            jax.ShapeDtypeStruct((1, own_cols), f32),
        ),
    )(solution, coeffs, ratio)
    return solution.T, coeffs.T, ratio[0]


def solution(mesh):
    return jax.shard_map(
        functools.partial(shards, mesh.shape["grp"]),
        mesh=mesh,
        in_specs=(P(("rows", "grp"), None), P(("rows", "grp"), None), P(), P(("rows", "grp"))),
        out_specs=(P(None, "grp"), P(None, "grp"), P("grp")),
        check_vma=False,
    )
```

```python
import functools

import jax
import jax.numpy as jnp
from jax import lax
from jax.experimental import pallas as pl
from jax.experimental.pallas import tpu as pltpu
from jax.sharding import PartitionSpec as P

ITERS = 3
FLOOR_SQ = 0.01
MESH = pl.DeviceIdType.MESH
SIDE = 4
CHIPS = SIDE * SIDE
LANES = 128
TILE = 256
GROUP = SIDE * LANES

SEND_ROWS = (2, 1, 3, 0)
SEND_COLS = (2, 1, 3, 0)
TAKE_ROWS = (2, 1, 3, 0)

NT = (((1,), (1,)), ((), ()))


def dot(a, b):
    return jnp.dot(a, b, preferred_element_type=jnp.float32)


def dot_nt(a, b):
    return lax.dot_general(a, b, NT, preferred_element_type=jnp.float32)


def wide(column, count):
    return jnp.concatenate([column] * count, axis=1)


def halves(value):
    high = value.astype(jnp.bfloat16)
    return high, (value - high.astype(jnp.float32)).astype(jnp.bfloat16)


def kernel(
    planes,
    count_ref, a_hbm, b_hbm, n_hbm,
    sol_ref, coef_ref, ratio_ref,
    a, b, n, bm, bt, raw, image, pref, pb, p0, q, part, partb, crecv, xsend, xrecv, ownrow, zbuf,
    live, csq, xsq, zsq, fsq, state, scalars, ucol, vcol, vinv, sums,
    load_sem, cs_sem, cr_sem, ps_sem, pr_sem, ls_sem, lr_sem, as_sem, ar_sem,
    xs_sem, xr_sem, zs_sem, zr_sem, gs_sem, gr_sem,
    xsqs_sem, xsqr_sem, zsqs_sem, zsqr_sem, fsqs_sem, fsqr_sem, ts_sem, tr_sem, us_sem, ur_sem,
):
    half, width = raw.shape
    columns = 2 * half
    rows = b.shape[0]
    both = 2 * rows
    own_cols = columns // planes
    per_core = planes // 2

    r = lax.axis_index("rows")
    z = lax.axis_index("grp")
    core = lax.rem(r, 2)
    chip = lax.div(r, 2)
    x = lax.rem(chip, SIDE)
    y = lax.div(chip, SIDE)

    def row_at(dy):
        return lax.rem(y + dy, SIDE)

    def chip_at(dy, dx):
        return row_at(dy) * SIDE + lax.rem(x + dx, SIDE)

    offsets = [(dy, dx) for dy in SEND_ROWS for dx in SEND_COLS if dy or dx]
    plane_chips = [chip_at(dy, dx) for dy, dx in offsets]
    other_planes = [lax.rem(z + k, planes) for k in sorted(range(1, planes), key=lambda k: -min(k, planes - k))]
    partner = {"rows": chip * 2 + (1 - core), "grp": z}

    def on_chip(c):
        return {"rows": c * 2 + core, "grp": z}

    def on_plane(k, other=False):
        return {"rows": chip * 2 + (1 - core) if other else r, "grp": k}

    def remote(src, dst, send, recv, device):
        return pltpu.make_async_remote_copy(
            src_ref=src, dst_ref=dst, send_sem=send, recv_sem=recv, device_id=device, device_id_type=MESH
        )

    barrier = pltpu.get_barrier_semaphore()
    partners = [on_plane(k, other) for k in other_planes for other in (False, True)]
    partners += [on_chip(c) for c in plane_chips] + [partner]
    for device in partners:
        pl.semaphore_signal(barrier, inc=1, device_id=device, device_id_type=MESH)

    load_b = pltpu.make_async_copy(b_hbm, b, load_sem.at[0])
    load_a = pltpu.make_async_copy(a_hbm, a.at[pl.ds(0, rows)], load_sem.at[1])
    load_n = pltpu.make_async_copy(n_hbm, n, load_sem.at[2])
    load_b.start()
    load_a.start()

    ours = pl.ds(pl.multiple_of(core * half, half), half)
    theirs = pl.ds(pl.multiple_of((1 - core) * half, half), half)
    ones = jnp.ones((8, both), jnp.bfloat16)

    core_copy = remote(partb.at[theirs], crecv, cs_sem, cr_sem, partner)
    residue_copy = remote(p0.at[theirs], p0.at[pl.ds(columns, half)], ps_sem, pr_sem, partner)
    live_copy = remote(live.at[0], live.at[1], ls_sem, lr_sem, partner)
    a_copy = remote(a.at[pl.ds(0, rows)], a.at[pl.ds(rows, rows)], as_sem, ar_sem, partner)
    state_copy = remote(state.at[core], state.at[core], ts_sem, tr_sem, partner)
    state_arrival = remote(state.at[1 - core], state.at[1 - core], ts_sem, tr_sem, partner)
    scalars_copy = remote(scalars.at[core], scalars.at[core], us_sem, ur_sem, partner)
    scalars_arrival = remote(scalars.at[1 - core], scalars.at[1 - core], us_sem, ur_sem, partner)

    def plane_copy(c):
        return remote(xsend.at[c], xrecv.at[chip], xs_sem.at[c], xr_sem.at[chip], on_chip(c))

    def plane_arrival(c):
        return remote(xsend.at[c], xrecv.at[c], xs_sem.at[c], xr_sem.at[c], on_chip(c))

    def plane_sq(c):
        return remote(xsq.at[chip], xsq.at[chip], xsqs_sem.at[c], xsqr_sem.at[chip], on_chip(c))

    def plane_sq_arrival(c):
        return remote(xsq.at[c], xsq.at[c], xsqs_sem.at[c], xsqr_sem.at[c], on_chip(c))

    def depth_copy(par, k):
        return remote(zbuf.at[par, z], zbuf.at[par, z], zs_sem.at[par, k], zr_sem.at[par, z], on_plane(k))

    def depth_arrival(par, k):
        return remote(zbuf.at[par, k], zbuf.at[par, k], zs_sem.at[par, k], zr_sem.at[par, k], on_plane(k))

    def depth_sq(par, k):
        return remote(zsq.at[par, z], zsq.at[par, z], zsqs_sem.at[par, k], zsqr_sem.at[par, z], on_plane(k))

    def depth_sq_arrival(par, k):
        return remote(zsq.at[par, k], zsq.at[par, k], zsqs_sem.at[par, k], zsqr_sem.at[par, k], on_plane(k))

    def last_sq(k, other):
        there = (1 - core) if other else core
        return remote(fsq.at[core, z], fsq.at[core, z], fsqs_sem.at[there, k], fsqr_sem.at[core, z], on_plane(k, other))

    def last_sq_arrival(h, k):
        return remote(fsq.at[h, k], fsq.at[h, k], fsqs_sem.at[h, k], fsqr_sem.at[h, k], partner)

    def piece(c):
        return q.at[:, pl.ds(pl.multiple_of(c * LANES, LANES), LANES)]

    def gather_copy(c):
        return remote(piece(chip), piece(chip), gs_sem.at[c], gr_sem.at[chip], on_chip(c))

    def gather_arrival(c):
        return remote(piece(c), piece(c), gs_sem.at[c], gr_sem.at[c], on_chip(c))

    def keep_squares():
        square = pref[...] * pref[...]
        blank = jnp.zeros_like(square)
        square = jnp.concatenate(
            [jnp.where(core == 0, square, blank), jnp.where(core == 0, blank, square)], axis=0
        )
        high, low = halves(square)
        total = dot_nt(ones, high) + dot_nt(ones, low)
        csq[...] = total[0:1]

    def squares_plane():
        xsq[chip] = csq[...]
        for c in plane_chips:
            plane_sq(c).start()

    def squares_of_plane():
        for c in plane_chips:
            plane_sq_arrival(c).wait_recv()
        total = xsq[0]
        for c in range(1, CHIPS):
            total = total + xsq[c]
        return total

    def keep_norm(total):
        spread = jnp.transpose(jnp.broadcast_to(total, (columns, columns)))
        ucol[...] = jnp.sqrt(spread + FLOOR_SQ)

    def send_group(value, dy):
        line = row_at(dy) * SIDE
        for s in range(SIDE):
            block = value[:, s * LANES : (s + 1) * LANES]
            xsend[line + s] = block.astype(jnp.bfloat16)
            if dy == 0:
                ownrow[s] = block
        for dx in SEND_COLS:
            if dy or dx:
                plane_copy(chip_at(dy, dx)).start()

    raw[...] = jnp.zeros_like(raw)
    vinv[...] = jnp.zeros_like(vinv)
    state[...] = jnp.zeros_like(state)
    scalars[...] = jnp.zeros_like(scalars)
    shown = (lax.broadcasted_iota(jnp.int32, (1, rows), 1) < count_ref[0]).astype(jnp.float32)
    live[0] = shown
    load_b.wait()
    first_residue = shown * jnp.transpose(b[...].astype(jnp.float32))
    p0[pl.ds(0, columns)] = first_residue.astype(jnp.bfloat16)
    load_a.wait()
    load_n.start()

    start_residue = p0[pl.ds(0, columns)]
    for j in range(width // TILE):
        lanes = slice(j * TILE, (j + 1) * TILE)
        product = dot(start_residue, a[pl.ds(0, rows), lanes])
        part[:, lanes] = product
        partb[:, lanes] = product.astype(jnp.bfloat16)
    pl.semaphore_wait(barrier, len(partners))
    core_copy.start()
    residue_copy.start()
    live_copy.start()
    a_copy.start()

    mine = pl.ds(pl.multiple_of(lax.rem(z, per_core) * own_cols, own_cols), own_cols)
    spread = width // LANES

    def recur(first):
        u_own = ucol[pl.ds(pl.multiple_of(core * half, half) + lax.rem(z, per_core) * own_cols, own_cols)]
        v_own = vcol[mine]
        rho, phi, start = (scalars[core, pl.ds(k * own_cols, own_cols)] for k in range(3))
        search = state[core, pl.ds(own_cols, own_cols)]
        radius = jnp.sqrt(rho * rho + u_own * u_own)
        cosine = rho / radius
        sine = u_own / radius
        state[core, pl.ds(0, own_cols)] = (
            state[core, pl.ds(0, own_cols)] + wide(cosine * phi / radius, spread) * search
        )
        state[core, pl.ds(own_cols, own_cols)] = raw[mine] * wide(vinv[mine], spread) - wide(sine * v_own / radius, spread) * search
        scalars[core, pl.ds(0, own_cols)] = jnp.where(first, v_own, -cosine * v_own)
        scalars[core, pl.ds(own_cols, own_cols)] = jnp.where(first, u_own, sine * phi)
        scalars[core, pl.ds(2 * own_cols, own_cols)] = jnp.where(first, u_own, start)

    def group(dy):
        return pl.ds(pl.multiple_of(row_at(dy) * GROUP, GROUP), GROUP)

    def group_arrival(dy):
        for dx in SEND_COLS:
            if dy or dx:
                gather_arrival(chip_at(dy, dx)).wait_recv()

    def folded(value):
        total = value[:, :LANES] * value[:, :LANES]
        for k in range(1, value.shape[1] // LANES):
            block = value[:, k * LANES : (k + 1) * LANES]
            total = total + block * block
        return total

    def multiply(first):
        lines = pl.ds(first, rows)

        def step(k, c):
            here = pl.ds(pl.multiple_of(k * 2 * TILE, 2 * TILE), 2 * TILE)
            bm[lines, here] = dot(a[lines], n[:, here]).astype(jnp.bfloat16)
            return c

        lax.fori_loop(0, width // (2 * TILE), step, 0)

    def flip():
        lines = lax.broadcasted_iota(jnp.int32, (TILE, TILE), 0)
        same = (lines == lax.broadcasted_iota(jnp.int32, (TILE, TILE), 1)).astype(jnp.bfloat16)

        def step(k, c):
            here = pl.ds(pl.multiple_of(k * TILE, TILE), TILE)
            for j in range(width // TILE):
                lanes = slice(j * TILE, (j + 1) * TILE)
                bt[lanes, here] = dot_nt(same, bm[here, lanes]).astype(jnp.bfloat16)
            return c

        lax.fori_loop(0, both // TILE, step, 0)

    def turn(i, carry):
        par = lax.rem(i, 2)

        @pl.when(i == 0)
        def _():
            core_copy.wait_recv()
            for dy in SEND_ROWS:
                lanes = pl.ds(pl.multiple_of(row_at(dy) * GROUP, GROUP), GROUP)
                send_group(part[ours, lanes] + crecv[:, lanes].astype(jnp.float32), dy)
            residue_copy.wait_recv()
            pref[...] = jnp.concatenate([p0[ours], p0[pl.ds(columns, half)]], axis=1).astype(jnp.float32)

        @pl.when(i > 0)
        def _():
            residue = pb[...]
            for dy in SEND_ROWS:
                lanes = pl.ds(pl.multiple_of(row_at(dy) * GROUP, GROUP), GROUP)
                send_group(dot(residue, bm[:, lanes]), dy)

        keep_squares()
        squares_plane()

        @pl.when(i > 0)
        def _():
            recur(i == 1)

        @pl.when(i == 0)
        def _():
            load_n.wait()
            multiply(0)

        own = ownrow[x]
        for c in plane_chips:
            plane_arrival(c).wait_recv()
            own = own + xrecv[c].astype(jnp.float32)
        zbuf[par, z] = own.astype(jnp.bfloat16)
        zsq[par, z] = squares_of_plane()
        for k in other_planes:
            depth_copy(par, k).start()
            depth_sq(par, k).start()

        @pl.when(i == 0)
        def _():
            a_copy.wait_recv()
            live_copy.wait_recv()
            multiply(rows)

        for k in other_planes:
            depth_sq_arrival(par, k).wait_recv()
        total = zsq[par, 0]
        for k in range(1, planes):
            total = total + zsq[par, k]
        keep_norm(total)
        u = ucol[ours]
        for k in other_planes:
            depth_arrival(par, k).wait_recv()
        total = zbuf[par, 0].astype(jnp.float32)
        for k in range(1, planes):
            total = total + zbuf[par, k].astype(jnp.float32)
        q[:, pl.ds(pl.multiple_of(chip * LANES, LANES), LANES)] = (total / u).astype(jnp.bfloat16)

        for c in plane_chips:
            gather_copy(c).start()

        @pl.when(i == 0)
        def _():
            flip()
            squares = jnp.zeros((half, LANES), jnp.float32)
            for taken, dy in enumerate(TAKE_ROWS):
                group_arrival(dy)
                here = group(dy)
                value = q[:, here]
                for j in range(width // TILE):
                    lanes = slice(j * TILE, (j + 1) * TILE)
                    product = dot(value, n[here, lanes])
                    if taken:
                        product = raw[:, lanes] + product
                    raw[:, lanes] = product
                    if taken == SIDE - 1:
                        squares = squares + folded(product)
            sums[...] = squares
            image[...] = dot(raw[...].astype(jnp.bfloat16), bt[...])

        @pl.when(i > 0)
        def _():
            back = wide(u * vinv[...], SIDE)
            squares = jnp.zeros((half, LANES), jnp.float32)
            for taken, dy in enumerate(TAKE_ROWS):
                group_arrival(dy)
                here = group(dy)
                value = q[:, here].astype(jnp.float32) - back * raw[:, here]
                raw[:, here] = value
                product = dot(value.astype(jnp.bfloat16), bt[here, :])
                image[...] = image[...] + product if taken else product
                squares = squares + folded(value)
            sums[...] = squares

        v = jnp.sqrt(jnp.sum(sums[...], axis=1, keepdims=True) + FLOOR_SQ)
        v = jnp.broadcast_to(v, (half, LANES))
        inverse = 1.0 / v
        vcol[...] = v
        vinv[...] = inverse

        scale, back = wide(inverse, rows // LANES), wide(v / u, rows // LANES)
        for h in range(2):
            lanes = slice(h * rows, (h + 1) * rows)
            residue = live[h] * (scale * image[:, lanes] - back * pref[:, lanes])
            pref[:, lanes] = residue
            pb[:, lanes] = residue.astype(jnp.bfloat16)

        for c in plane_chips:
            plane_copy(c).wait_send()
            plane_sq(c).wait_send()

        for k in other_planes:
            depth_copy(par, k).wait_send()
            depth_sq(par, k).wait_send()
        for c in plane_chips:
            gather_copy(c).wait_send()
        return carry

    lax.fori_loop(0, ITERS, turn, 0)

    keep_squares()
    squares_plane()
    recur(ITERS == 1)
    fsq[core, z] = squares_of_plane()
    last_core = remote(fsq.at[core, z], fsq.at[core, z], fsqs_sem.at[1 - core, z], fsqr_sem.at[core, z], partner)
    for k in other_planes:
        last_sq(k, False).start()
        last_sq(k, True).start()
    last_core.start()
    state_copy.start()
    scalars_copy.start()

    holder = lax.div(z, per_core)
    state_arrival.wait_recv()
    scalars_arrival.wait_recv()
    high, low = halves(state[holder])
    stacked = jnp.concatenate([high, low], axis=0)
    for j in range(width // TILE):
        lanes = slice(j * TILE, (j + 1) * TILE)
        product = dot_nt(stacked, n[lanes, :])
        raw[pl.ds(0, 2 * own_cols), lanes] = product[: 2 * own_cols] + product[2 * own_cols :]

    last_sq_arrival(1 - core, z).wait_recv()
    for k in other_planes:
        last_sq_arrival(0, k).wait_recv()
        last_sq_arrival(1, k).wait_recv()
    total = fsq[0, 0]
    for h in range(2):
        for k in range(planes):
            if h or k:
                total = total + fsq[h, k]
    keep_norm(total)
    u_own = ucol[pl.ds(pl.multiple_of(z * own_cols, own_cols), own_cols)]
    rho, phi, start = (scalars[holder, pl.ds(k * own_cols, own_cols)] for k in range(3))
    radius = jnp.sqrt(rho * rho + u_own * u_own)
    cosine = rho / radius
    sine = u_own / radius
    step = wide(cosine * phi / radius, spread)
    coef_ref[...] = state[holder, pl.ds(0, own_cols)] + step * state[holder, pl.ds(own_cols, own_cols)]
    sol_ref[...] = raw[pl.ds(0, own_cols)] + step * raw[pl.ds(own_cols, own_cols)]
    ratio_ref[...] = sine * phi / start

    for copy in (core_copy, residue_copy, live_copy, a_copy, state_copy, scalars_copy, last_core):
        copy.wait_send()
    for c in plane_chips:
        plane_sq(c).wait_send()
    for k in other_planes:
        last_sq(k, False).wait_send()
        last_sq(k, True).wait_send()


def finish(sol_in, coef_in, ratio_in, sol_ref, coef_ref, ratio_ref):
    sol_ref[...] = sol_in[...]
    coef_ref[...] = coef_in[...]
    ratio = ratio_in[...]
    square = jnp.concatenate([ratio] * (LANES // ratio.shape[0]), axis=0)
    ratio_ref[...] = jnp.transpose(square)[0:1, : ratio.shape[0]]


def shards(planes, matrix, right_side, precond, row_counts):
    rows, width = matrix.shape
    columns = right_side.shape[1]
    own_cols = columns // planes
    half = columns // 2
    vmem, dma = pltpu.VMEM, pltpu.SemaphoreType.DMA
    bf16, f32 = jnp.bfloat16, jnp.float32
    solution, coeffs, ratio = pl.pallas_call(
        functools.partial(kernel, planes),
        out_shape=(
            jax.ShapeDtypeStruct((own_cols, width), f32),
            jax.ShapeDtypeStruct((own_cols, width), f32),
            jax.ShapeDtypeStruct((own_cols, LANES), f32),
        ),
        in_specs=[pl.BlockSpec(memory_space=pltpu.SMEM)] + [pl.BlockSpec(memory_space=pl.ANY)] * 3,
        out_specs=(pl.BlockSpec(memory_space=vmem),) * 3,
        scratch_shapes=[
            vmem((2 * rows, width), bf16),
            vmem((rows, columns), bf16),
            vmem((width, width), bf16),
            vmem((2 * rows, width), bf16),
            vmem((width, 2 * rows), bf16),
            vmem((half, width), f32),
            vmem((half, 2 * rows), f32),
            vmem((half, 2 * rows), f32),
            vmem((half, 2 * rows), bf16),
            vmem((columns + half, rows), bf16),
            vmem((half, width), bf16),
            vmem((columns, width), f32),
            vmem((columns, width), bf16),
            vmem((half, width), bf16),
            vmem((CHIPS, half, LANES), bf16),
            vmem((CHIPS, half, LANES), bf16),
            vmem((SIDE, half, LANES), f32),
            vmem((2, planes, half, LANES), bf16),
            vmem((2, 1, rows), f32),
            vmem((1, columns), f32),
            vmem((CHIPS, 1, columns), f32),
            vmem((2, planes, 1, columns), f32),
            vmem((2, planes, 1, columns), f32),
            vmem((2, 2 * own_cols, width), f32),
            vmem((2, 3 * own_cols, LANES), f32),
            vmem((columns, LANES), f32),
            vmem((half, LANES), f32),
            vmem((half, LANES), f32),
            vmem((half, LANES), f32),
            dma((3,)),
            dma, dma, dma, dma, dma, dma, dma, dma,
            dma((CHIPS,)), dma((CHIPS,)),
            dma((2, planes)), dma((2, planes)),
            dma((CHIPS,)), dma((CHIPS,)),
            dma((CHIPS,)), dma((CHIPS,)),
            dma((2, planes)), dma((2, planes)),
            dma((2, planes)), dma((2, planes)),
            dma, dma, dma, dma,
        ],
        compiler_params=pltpu.CompilerParams(
            collective_id=0, has_side_effects=True, vmem_limit_bytes=60 * 1024 * 1024
        ),
    )(row_counts, matrix, right_side, precond)
    solution, coeffs, ratio = pl.pallas_call(
        finish,
        out_shape=(
            jax.ShapeDtypeStruct((own_cols, width), f32),
            jax.ShapeDtypeStruct((own_cols, width), f32),
            jax.ShapeDtypeStruct((1, own_cols), f32),
        ),
    )(solution, coeffs, ratio)
    return solution.T, coeffs.T, ratio[0]


def solution(mesh):
    return jax.shard_map(
        functools.partial(shards, mesh.shape["grp"]),
        mesh=mesh,
        in_specs=(P(("rows", "grp"), None), P(("rows", "grp"), None), P(), P(("rows", "grp"))),
        out_specs=(P(None, "grp"), P(None, "grp"), P("grp")),
        check_vma=False,
    )
```

```python
import functools

import jax
import jax.numpy as jnp
from jax import lax
from jax.experimental import pallas as pl
from jax.experimental.pallas import tpu as pltpu
from jax.sharding import PartitionSpec as P

ITERS = 3
FLOOR_SQ = 0.01
MESH = pl.DeviceIdType.MESH
SIDE = 4
CHIPS = SIDE * SIDE
LANES = 128
TILE = 256
PARTS = 1
GROUP = SIDE * LANES

SEND_ROWS = (2, 1, 3, 0)
SEND_COLS = (2, 1, 3, 0)
TAKE_ROWS = (2, 1, 3, 0)

NT = (((1,), (1,)), ((), ()))


def dot(a, b):
    return jnp.dot(a, b, preferred_element_type=jnp.float32)


def dot_nt(a, b):
    return lax.dot_general(a, b, NT, preferred_element_type=jnp.float32)


def wide(column, count):
    return jnp.concatenate([column] * count, axis=1)


def halves(value):
    high = value.astype(jnp.bfloat16)
    return high, (value - high.astype(jnp.float32)).astype(jnp.bfloat16)


def kernel(
    planes,
    count_hbm, a_hbm, b_hbm, n_hbm,
    sol_ref, coef_ref, ratio_ref,
    count, a, b, n, bm, bt, raw, image, pref, pb, p0, q, part, partb, crecv, xsend, xrecv, ownrow, zbuf,
    live, csq, xsq, zsq, fsq, state, scalars, ucol, vcol, vinv, sums,
    load_sem, cs_sem, cr_sem, ps_sem, pr_sem, ls_sem, lr_sem, as_sem, ar_sem,
    xs_sem, xr_sem, zs_sem, zr_sem, gs_sem, gr_sem,
    xsqs_sem, xsqr_sem, zsqs_sem, zsqr_sem, fsqs_sem, fsqr_sem, ts_sem, tr_sem, us_sem, ur_sem,
):
    half, width = raw.shape
    columns = 2 * half
    rows = b.shape[0]
    both = 2 * rows
    own_cols = columns // planes
    per_core = planes // 2

    r = lax.axis_index("rows")
    z = lax.axis_index("grp")
    core = lax.rem(r, 2)
    chip = lax.div(r, 2)
    x = lax.rem(chip, SIDE)
    y = lax.div(chip, SIDE)

    def row_at(dy):
        return lax.rem(y + dy, SIDE)

    def chip_at(dy, dx):
        return row_at(dy) * SIDE + lax.rem(x + dx, SIDE)

    offsets = [(dy, dx) for dy in SEND_ROWS for dx in SEND_COLS if dy or dx]
    plane_chips = [chip_at(dy, dx) for dy, dx in offsets]
    other_planes = [lax.rem(z + k, planes) for k in sorted(range(1, planes), key=lambda k: -min(k, planes - k))]
    partner = {"rows": chip * 2 + (1 - core), "grp": z}

    def on_chip(c):
        return {"rows": c * 2 + core, "grp": z}

    def on_plane(k, other=False):
        return {"rows": chip * 2 + (1 - core) if other else r, "grp": k}

    def remote(src, dst, send, recv, device):
        return pltpu.make_async_remote_copy(
            src_ref=src, dst_ref=dst, send_sem=send, recv_sem=recv, device_id=device, device_id_type=MESH
        )

    barrier = pltpu.get_barrier_semaphore()
    partners = [on_plane(k, other) for k in other_planes for other in (False, True)]
    partners += [on_chip(c) for c in plane_chips] + [partner]
    for device in partners:
        pl.semaphore_signal(barrier, inc=1, device_id=device, device_id_type=MESH)

    load_b = pltpu.make_async_copy(b_hbm, b, load_sem.at[0])
    load_a = pltpu.make_async_copy(a_hbm, a.at[pl.ds(0, rows)], load_sem.at[1])
    load_n = pltpu.make_async_copy(n_hbm, n, load_sem.at[2])
    load_count = pltpu.make_async_copy(count_hbm, count, load_sem.at[3])
    load_count.start()
    load_b.start()
    load_a.start()

    ours = pl.ds(pl.multiple_of(core * half, half), half)
    theirs = pl.ds(pl.multiple_of((1 - core) * half, half), half)
    ones = jnp.ones((8, both), jnp.bfloat16)

    def group(dy):
        return pl.ds(pl.multiple_of(row_at(dy) * GROUP, GROUP), GROUP)

    def core_copy(dy):
        return remote(partb.at[theirs, group(dy)], crecv.at[:, group(dy)], cs_sem.at[dy], cr_sem.at[dy], partner)

    residue_copy = remote(p0.at[theirs], p0.at[pl.ds(columns, half)], ps_sem, pr_sem, partner)
    live_copy = remote(live.at[0], live.at[1], ls_sem, lr_sem, partner)
    a_copy = remote(a.at[pl.ds(0, rows)], a.at[pl.ds(rows, rows)], as_sem, ar_sem, partner)
    state_copy = remote(state.at[core], state.at[core], ts_sem, tr_sem, partner)
    state_arrival = remote(state.at[1 - core], state.at[1 - core], ts_sem, tr_sem, partner)
    scalars_copy = remote(scalars.at[core], scalars.at[core], us_sem, ur_sem, partner)
    scalars_arrival = remote(scalars.at[1 - core], scalars.at[1 - core], us_sem, ur_sem, partner)

    part_rows = half // PARTS

    def part_of(g):
        return pl.ds(g * part_rows, part_rows)

    def plane_copy(c, g):
        mine_at, there = xsend.at[c, part_of(g)], xrecv.at[chip, part_of(g)]
        return remote(mine_at, there, xs_sem.at[c, g], xr_sem.at[chip, g], on_chip(c))

    def plane_arrival(c, g):
        mine_at, here = xsend.at[c, part_of(g)], xrecv.at[c, part_of(g)]
        return remote(mine_at, here, xs_sem.at[c, g], xr_sem.at[c, g], on_chip(c))

    def plane_sq(c):
        return remote(xsq.at[chip], xsq.at[chip], xsqs_sem.at[c], xsqr_sem.at[chip], on_chip(c))

    def plane_sq_arrival(c):
        return remote(xsq.at[c], xsq.at[c], xsqs_sem.at[c], xsqr_sem.at[c], on_chip(c))

    def depth_copy(par, k, g):
        block = zbuf.at[par, z, part_of(g)]
        return remote(block, block, zs_sem.at[par, k, g], zr_sem.at[par, z, g], on_plane(k))

    def depth_arrival(par, k, g):
        block = zbuf.at[par, k, part_of(g)]
        return remote(block, block, zs_sem.at[par, k, g], zr_sem.at[par, k, g], on_plane(k))

    def depth_sq(par, k):
        return remote(zsq.at[par, z], zsq.at[par, z], zsqs_sem.at[par, k], zsqr_sem.at[par, z], on_plane(k))

    def depth_sq_arrival(par, k):
        return remote(zsq.at[par, k], zsq.at[par, k], zsqs_sem.at[par, k], zsqr_sem.at[par, k], on_plane(k))

    def last_sq(k, other):
        there = (1 - core) if other else core
        return remote(fsq.at[core, z], fsq.at[core, z], fsqs_sem.at[there, k], fsqr_sem.at[core, z], on_plane(k, other))

    def last_sq_arrival(h, k):
        return remote(fsq.at[h, k], fsq.at[h, k], fsqs_sem.at[h, k], fsqr_sem.at[h, k], partner)

    def piece(c, g):
        return q.at[part_of(g), pl.ds(pl.multiple_of(c * LANES, LANES), LANES)]

    def gather_copy(c, g):
        return remote(piece(chip, g), piece(chip, g), gs_sem.at[c, g], gr_sem.at[chip, g], on_chip(c))

    def gather_arrival(c, g):
        return remote(piece(c, g), piece(c, g), gs_sem.at[c, g], gr_sem.at[c, g], on_chip(c))

    def keep_squares():
        square = pref[...] * pref[...]
        blank = jnp.zeros_like(square)
        square = jnp.concatenate(
            [jnp.where(core == 0, square, blank), jnp.where(core == 0, blank, square)], axis=0
        )
        high, low = halves(square)
        total = dot_nt(ones, high) + dot_nt(ones, low)
        csq[...] = total[0:1]

    def squares_plane():
        xsq[chip] = csq[...]
        for c in plane_chips:
            plane_sq(c).start()

    def squares_of_plane():
        for c in plane_chips:
            plane_sq_arrival(c).wait_recv()
        total = xsq[0]
        for c in range(1, CHIPS):
            total = total + xsq[c]
        return total

    def keep_norm(total):
        spread = jnp.transpose(jnp.broadcast_to(total, (columns, columns)))
        ucol[...] = jnp.sqrt(spread + FLOOR_SQ)

    def send_group(value, dy):
        line = row_at(dy) * SIDE
        for s in range(SIDE):
            block = value[:, s * LANES : (s + 1) * LANES]
            xsend[line + s] = block.astype(jnp.bfloat16)
            if dy == 0:
                ownrow[s] = block
        for dx in SEND_COLS:
            if dy or dx:
                plane_copy(chip_at(dy, dx), 0).start()

    raw[...] = jnp.zeros_like(raw)
    vinv[...] = jnp.zeros_like(vinv)
    state[...] = jnp.zeros_like(state)
    scalars[...] = jnp.zeros_like(scalars)
    load_count.wait()
    shown = (lax.broadcasted_iota(jnp.int32, (1, rows), 1) < count[0]).astype(jnp.float32)
    live[0] = shown
    load_b.wait()
    first_residue = shown * jnp.transpose(b[...].astype(jnp.float32))
    p0[pl.ds(0, columns)] = first_residue.astype(jnp.bfloat16)
    load_a.wait()
    load_n.start()

    start_residue = p0[pl.ds(0, columns)]
    for j in range(width // TILE):
        lanes = slice(j * TILE, (j + 1) * TILE)
        product = dot(start_residue, a[pl.ds(0, rows), lanes])
        part[:, lanes] = product
        partb[:, lanes] = product.astype(jnp.bfloat16)
    pl.semaphore_wait(barrier, len(partners))
    for dy in SEND_ROWS:
        core_copy(dy).start()
    residue_copy.start()
    live_copy.start()
    a_copy.start()

    mine = pl.ds(pl.multiple_of(lax.rem(z, per_core) * own_cols, own_cols), own_cols)
    spread = width // LANES

    def recur(first):
        u_own = ucol[pl.ds(pl.multiple_of(core * half, half) + lax.rem(z, per_core) * own_cols, own_cols)]
        v_own = vcol[mine]
        rho, phi, start = (scalars[core, pl.ds(k * own_cols, own_cols)] for k in range(3))
        search = state[core, pl.ds(own_cols, own_cols)]
        radius = jnp.sqrt(rho * rho + u_own * u_own)
        cosine = rho / radius
        sine = u_own / radius
        state[core, pl.ds(0, own_cols)] = (
            state[core, pl.ds(0, own_cols)] + wide(cosine * phi / radius, spread) * search
        )
        state[core, pl.ds(own_cols, own_cols)] = raw[mine] * wide(vinv[mine], spread) - wide(sine * v_own / radius, spread) * search
        scalars[core, pl.ds(0, own_cols)] = jnp.where(first, v_own, -cosine * v_own)
        scalars[core, pl.ds(own_cols, own_cols)] = jnp.where(first, u_own, sine * phi)
        scalars[core, pl.ds(2 * own_cols, own_cols)] = jnp.where(first, u_own, start)

    def group_arrival(dy):
        for dx in SEND_COLS:
            if dy or dx:
                for g in range(PARTS):
                    gather_arrival(chip_at(dy, dx), g).wait_recv()

    def folded(value):
        total = value[:, :LANES] * value[:, :LANES]
        for k in range(1, value.shape[1] // LANES):
            block = value[:, k * LANES : (k + 1) * LANES]
            total = total + block * block
        return total

    def multiply(first):
        lines = pl.ds(first, rows)

        def step(k, c):
            here = pl.ds(pl.multiple_of(k * 2 * TILE, 2 * TILE), 2 * TILE)
            bm[lines, here] = dot(a[lines], n[:, here]).astype(jnp.bfloat16)
            return c

        lax.fori_loop(0, width // (2 * TILE), step, 0)

    def flip():
        lines = lax.broadcasted_iota(jnp.int32, (TILE, TILE), 0)
        same = (lines == lax.broadcasted_iota(jnp.int32, (TILE, TILE), 1)).astype(jnp.bfloat16)

        def step(k, c):
            here = pl.ds(pl.multiple_of(k * TILE, TILE), TILE)
            for j in range(width // TILE):
                lanes = slice(j * TILE, (j + 1) * TILE)
                bt[lanes, here] = dot_nt(same, bm[here, lanes]).astype(jnp.bfloat16)
            return c

        lax.fori_loop(0, both // TILE, step, 0)

    def turn(i, carry):
        par = lax.rem(i, 2)

        @pl.when(i == 0)
        def _():
            for dy in SEND_ROWS:
                core_copy(dy).wait_recv()
                lanes = pl.ds(pl.multiple_of(row_at(dy) * GROUP, GROUP), GROUP)
                send_group(part[ours, lanes] + crecv[:, lanes].astype(jnp.float32), dy)
            residue_copy.wait_recv()
            pref[...] = jnp.concatenate([p0[ours], p0[pl.ds(columns, half)]], axis=1).astype(jnp.float32)

        @pl.when(i > 0)
        def _():
            residue = pb[...]
            for dy in SEND_ROWS:
                lanes = pl.ds(pl.multiple_of(row_at(dy) * GROUP, GROUP), GROUP)
                send_group(dot(residue, bm[:, lanes]), dy)

        for g in range(1, PARTS):
            for c in plane_chips:
                plane_copy(c, g).start()
        keep_squares()
        squares_plane()

        @pl.when(i > 0)
        def _():
            recur(i == 1)

        @pl.when(i == 0)
        def _():
            load_n.wait()
            multiply(0)

        for g in range(PARTS):
            own = ownrow[x, part_of(g)]
            for c in plane_chips:
                plane_arrival(c, g).wait_recv()
                own = own + xrecv[c, part_of(g)].astype(jnp.float32)
            zbuf[par, z, part_of(g)] = own.astype(jnp.bfloat16)
            for k in other_planes:
                depth_copy(par, k, g).start()
        zsq[par, z] = squares_of_plane()
        for k in other_planes:
            depth_sq(par, k).start()

        @pl.when(i == 0)
        def _():
            a_copy.wait_recv()
            live_copy.wait_recv()
            multiply(rows)

        for g in range(PARTS):
            for k in other_planes:
                depth_arrival(par, k, g).wait_recv()
            total = zbuf[par, 0, part_of(g)].astype(jnp.float32)
            for k in range(1, planes):
                total = total + zbuf[par, k, part_of(g)].astype(jnp.float32)
            q[part_of(g), pl.ds(pl.multiple_of(chip * LANES, LANES), LANES)] = total.astype(jnp.bfloat16)

            for c in plane_chips:
                gather_copy(c, g).start()
        for k in other_planes:
            depth_sq_arrival(par, k).wait_recv()
        total = zsq[par, 0]
        for k in range(1, planes):
            total = total + zsq[par, k]
        keep_norm(total)
        u = ucol[ours]
        shrink = 1.0 / u

        @pl.when(i == 0)
        def _():
            flip()
            squares = jnp.zeros((half, LANES), jnp.float32)
            for taken, dy in enumerate(TAKE_ROWS):
                group_arrival(dy)
                here = group(dy)
                value = q[:, here]
                for j in range(width // TILE):
                    lanes = slice(j * TILE, (j + 1) * TILE)
                    product = dot(value, n[here, lanes])
                    if taken:
                        product = raw[:, lanes] + product
                    if taken == SIDE - 1:
                        product = product * wide(shrink, TILE // LANES)
                    raw[:, lanes] = product
                    if taken == SIDE - 1:
                        squares = squares + folded(product)
            sums[...] = squares
            image[...] = dot(raw[...].astype(jnp.bfloat16), bt[...])

        @pl.when(i > 0)
        def _():
            back = wide(u * vinv[...], SIDE)
            squares = jnp.zeros((half, LANES), jnp.float32)
            for taken, dy in enumerate(TAKE_ROWS):
                group_arrival(dy)
                here = group(dy)
                value = wide(shrink, SIDE) * q[:, here].astype(jnp.float32) - back * raw[:, here]
                raw[:, here] = value
                product = dot(value.astype(jnp.bfloat16), bt[here, :])
                image[...] = image[...] + product if taken else product
                squares = squares + folded(value)
            sums[...] = squares

        v = jnp.sqrt(jnp.sum(sums[...], axis=1, keepdims=True) + FLOOR_SQ)
        v = jnp.broadcast_to(v, (half, LANES))
        inverse = 1.0 / v
        vcol[...] = v
        vinv[...] = inverse

        scale, back = wide(inverse, rows // LANES), wide(v / u, rows // LANES)
        for h in range(2):
            lanes = slice(h * rows, (h + 1) * rows)
            residue = live[h] * (scale * image[:, lanes] - back * pref[:, lanes])
            pref[:, lanes] = residue
            pb[:, lanes] = residue.astype(jnp.bfloat16)

        for c in plane_chips:
            for g in range(PARTS):
                plane_copy(c, g).wait_send()
            plane_sq(c).wait_send()

        for k in other_planes:
            for g in range(PARTS):
                depth_copy(par, k, g).wait_send()
            depth_sq(par, k).wait_send()
        for c in plane_chips:
            for g in range(PARTS):
                gather_copy(c, g).wait_send()
        return carry

    lax.fori_loop(0, ITERS, turn, 0)

    keep_squares()
    squares_plane()
    recur(ITERS == 1)
    fsq[core, z] = squares_of_plane()
    last_core = remote(fsq.at[core, z], fsq.at[core, z], fsqs_sem.at[1 - core, z], fsqr_sem.at[core, z], partner)
    for k in other_planes:
        last_sq(k, False).start()
        last_sq(k, True).start()
    last_core.start()
    state_copy.start()
    scalars_copy.start()

    holder = lax.div(z, per_core)
    state_arrival.wait_recv()
    scalars_arrival.wait_recv()
    high, low = halves(state[holder])
    stacked = jnp.concatenate([high, low], axis=0)
    for j in range(width // TILE):
        lanes = slice(j * TILE, (j + 1) * TILE)
        product = dot_nt(stacked, n[lanes, :])
        raw[pl.ds(0, 2 * own_cols), lanes] = product[: 2 * own_cols] + product[2 * own_cols :]

    last_sq_arrival(1 - core, z).wait_recv()
    for k in other_planes:
        last_sq_arrival(0, k).wait_recv()
        last_sq_arrival(1, k).wait_recv()
    total = fsq[0, 0]
    for h in range(2):
        for k in range(planes):
            if h or k:
                total = total + fsq[h, k]
    keep_norm(total)
    u_own = ucol[pl.ds(pl.multiple_of(z * own_cols, own_cols), own_cols)]
    rho, phi, start = (scalars[holder, pl.ds(k * own_cols, own_cols)] for k in range(3))
    radius = jnp.sqrt(rho * rho + u_own * u_own)
    cosine = rho / radius
    sine = u_own / radius
    step = wide(cosine * phi / radius, spread)
    coef_ref[...] = state[holder, pl.ds(0, own_cols)] + step * state[holder, pl.ds(own_cols, own_cols)]
    sol_ref[...] = raw[pl.ds(0, own_cols)] + step * raw[pl.ds(own_cols, own_cols)]
    ratio_ref[...] = sine * phi / start

    for dy in SEND_ROWS:
        core_copy(dy).wait_send()
    for copy in (residue_copy, live_copy, a_copy, state_copy, scalars_copy, last_core):
        copy.wait_send()
    for c in plane_chips:
        plane_sq(c).wait_send()
    for k in other_planes:
        last_sq(k, False).wait_send()
        last_sq(k, True).wait_send()


def finish(sol_in, coef_in, ratio_in, sol_ref, coef_ref, ratio_ref):
    sol_ref[...] = sol_in[...]
    coef_ref[...] = coef_in[...]
    ratio = ratio_in[...]
    square = jnp.concatenate([ratio] * (LANES // ratio.shape[0]), axis=0)
    ratio_ref[...] = jnp.transpose(square)[0:1, : ratio.shape[0]]


def shards(planes, matrix, right_side, precond, row_counts):
    rows, width = matrix.shape
    columns = right_side.shape[1]
    own_cols = columns // planes
    half = columns // 2
    vmem, dma = pltpu.VMEM, pltpu.SemaphoreType.DMA
    bf16, f32 = jnp.bfloat16, jnp.float32
    solution, coeffs, ratio = pl.pallas_call(
        functools.partial(kernel, planes),
        out_shape=(
            jax.ShapeDtypeStruct((own_cols, width), f32),
            jax.ShapeDtypeStruct((own_cols, width), f32),
            jax.ShapeDtypeStruct((own_cols, LANES), f32),
        ),
        in_specs=[pl.BlockSpec(memory_space=pl.ANY)] * 4,
        out_specs=(pl.BlockSpec(memory_space=vmem),) * 3,
        scratch_shapes=[
            pltpu.SMEM((1,), jnp.int32),
            vmem((2 * rows, width), bf16),
            vmem((rows, columns), bf16),
            vmem((width, width), bf16),
            vmem((2 * rows, width), bf16),
            vmem((width, 2 * rows), bf16),
            vmem((half, width), f32),
            vmem((half, 2 * rows), f32),
            vmem((half, 2 * rows), f32),
            vmem((half, 2 * rows), bf16),
            vmem((columns + half, rows), bf16),
            vmem((half, width), bf16),
            vmem((columns, width), f32),
            vmem((columns, width), bf16),
            vmem((half, width), bf16),
            vmem((CHIPS, half, LANES), bf16),
            vmem((CHIPS, half, LANES), bf16),
            vmem((SIDE, half, LANES), f32),
            vmem((2, planes, half, LANES), bf16),
            vmem((2, 1, rows), f32),
            vmem((1, columns), f32),
            vmem((CHIPS, 1, columns), f32),
            vmem((2, planes, 1, columns), f32),
            vmem((2, planes, 1, columns), f32),
            vmem((2, 2 * own_cols, width), f32),
            vmem((2, 3 * own_cols, LANES), f32),
            vmem((columns, LANES), f32),
            vmem((half, LANES), f32),
            vmem((half, LANES), f32),
            vmem((half, LANES), f32),
            dma((4,)),
            dma((SIDE,)), dma((SIDE,)), dma, dma, dma, dma, dma, dma,
            dma((CHIPS, PARTS)), dma((CHIPS, PARTS)),
            dma((2, planes, PARTS)), dma((2, planes, PARTS)),
            dma((CHIPS, PARTS)), dma((CHIPS, PARTS)),
            dma((CHIPS,)), dma((CHIPS,)),
            dma((2, planes)), dma((2, planes)),
            dma((2, planes)), dma((2, planes)),
            dma, dma, dma, dma,
        ],
        compiler_params=pltpu.CompilerParams(
            collective_id=0, has_side_effects=True, vmem_limit_bytes=60 * 1024 * 1024
        ),
    )(row_counts, matrix, right_side, precond)
    solution, coeffs, ratio = pl.pallas_call(
        finish,
        out_shape=(
            jax.ShapeDtypeStruct((own_cols, width), f32),
            jax.ShapeDtypeStruct((own_cols, width), f32),
            jax.ShapeDtypeStruct((1, own_cols), f32),
        ),
    )(solution, coeffs, ratio)
    return solution.T, coeffs.T, ratio[0]


def solution(mesh):
    return jax.shard_map(
        functools.partial(shards, mesh.shape["grp"]),
        mesh=mesh,
        in_specs=(P(("rows", "grp"), None), P(("rows", "grp"), None), P(), P(("rows", "grp"))),
        out_specs=(P(None, "grp"), P(None, "grp"), P("grp")),
        check_vma=False,
    )
```

```python
import functools

import jax
import jax.numpy as jnp
from jax import lax
from jax.experimental import pallas as pl
from jax.experimental.pallas import tpu as pltpu
from jax.sharding import PartitionSpec as P

ITERS = 3
FLOOR_SQ = 0.01
MESH = pl.DeviceIdType.MESH
SIDE = 4
CHIPS = SIDE * SIDE
LANES = 128
TILE = 256
PARTS = 1
GROUP = SIDE * LANES

SEND_ROWS = (2, 1, 3, 0)
SEND_COLS = (2, 1, 3, 0)
TAKE_ROWS = (2, 1, 3, 0)

NT = (((1,), (1,)), ((), ()))


def dot(a, b):
    return jnp.dot(a, b, preferred_element_type=jnp.float32)


def dot_nt(a, b):
    return lax.dot_general(a, b, NT, preferred_element_type=jnp.float32)


def wide(column, count):
    return jnp.concatenate([column] * count, axis=1)


def halves(value):
    high = value.astype(jnp.bfloat16)
    return high, (value - high.astype(jnp.float32)).astype(jnp.bfloat16)


def kernel(
    planes,
    count_hbm, a_hbm, b_hbm, n_hbm,
    sol_ref, coef_ref, ratio_ref,
    count, a, b, n, bm, bt, raw, image, pref, pb, p0, q, part, partb, crecv, xsend, xrecv, ownrow, zbuf,
    live, csq, xsq, zsq, fsq, state, scalars, ucol, vcol, vinv, sums,
    load_sem, cs_sem, cr_sem, ps_sem, pr_sem, ls_sem, lr_sem, as_sem, ar_sem,
    xs_sem, xr_sem, zs_sem, zr_sem, gs_sem, gr_sem,
    xsqs_sem, xsqr_sem, zsqs_sem, zsqr_sem, fsqs_sem, fsqr_sem, ts_sem, tr_sem, us_sem, ur_sem,
):
    half, width = raw.shape
    columns = 2 * half
    rows = b.shape[0]
    both = 2 * rows
    own_cols = columns // planes
    per_core = planes // 2

    r = lax.axis_index("rows")
    z = lax.axis_index("grp")
    core = lax.rem(r, 2)
    chip = lax.div(r, 2)
    x = lax.rem(chip, SIDE)
    y = lax.div(chip, SIDE)

    def row_at(dy):
        return lax.rem(y + dy, SIDE)

    def chip_at(dy, dx):
        return row_at(dy) * SIDE + lax.rem(x + dx, SIDE)

    offsets = [(dy, dx) for dy in SEND_ROWS for dx in SEND_COLS if dy or dx]
    plane_chips = [chip_at(dy, dx) for dy, dx in offsets]
    other_planes = [lax.rem(z + k, planes) for k in sorted(range(1, planes), key=lambda k: -min(k, planes - k))]
    partner = {"rows": chip * 2 + (1 - core), "grp": z}

    def on_chip(c):
        return {"rows": c * 2 + core, "grp": z}

    def on_plane(k, other=False):
        return {"rows": chip * 2 + (1 - core) if other else r, "grp": k}

    def remote(src, dst, send, recv, device):
        return pltpu.make_async_remote_copy(
            src_ref=src, dst_ref=dst, send_sem=send, recv_sem=recv, device_id=device, device_id_type=MESH
        )

    barrier = pltpu.get_barrier_semaphore()
    partners = [on_plane(k, other) for k in other_planes for other in (False, True)]
    partners += [on_chip(c) for c in plane_chips] + [partner]
    for device in partners:
        pl.semaphore_signal(barrier, inc=1, device_id=device, device_id_type=MESH)

    load_b = pltpu.make_async_copy(b_hbm, b, load_sem.at[0])
    load_a = pltpu.make_async_copy(a_hbm, a.at[pl.ds(0, rows)], load_sem.at[1])
    load_n = pltpu.make_async_copy(n_hbm, n, load_sem.at[2])
    load_count = pltpu.make_async_copy(count_hbm, count, load_sem.at[3])
    load_count.start()
    load_b.start()
    load_a.start()

    ours = pl.ds(pl.multiple_of(core * half, half), half)
    theirs = pl.ds(pl.multiple_of((1 - core) * half, half), half)
    ones = jnp.ones((8, both), jnp.bfloat16)

    def group(dy):
        return pl.ds(pl.multiple_of(row_at(dy) * GROUP, GROUP), GROUP)

    def core_copy(dy):
        return remote(partb.at[theirs, group(dy)], crecv.at[:, group(dy)], cs_sem.at[dy], cr_sem.at[dy], partner)

    residue_copy = remote(p0.at[theirs], p0.at[pl.ds(columns, half)], ps_sem, pr_sem, partner)
    live_copy = remote(live.at[0], live.at[1], ls_sem, lr_sem, partner)
    a_copy = remote(a.at[pl.ds(0, rows)], a.at[pl.ds(rows, rows)], as_sem, ar_sem, partner)
    state_copy = remote(state.at[core], state.at[core], ts_sem, tr_sem, partner)
    state_arrival = remote(state.at[1 - core], state.at[1 - core], ts_sem, tr_sem, partner)
    scalars_copy = remote(scalars.at[core], scalars.at[core], us_sem, ur_sem, partner)
    scalars_arrival = remote(scalars.at[1 - core], scalars.at[1 - core], us_sem, ur_sem, partner)

    part_rows = half // PARTS

    def part_of(g):
        return pl.ds(g * part_rows, part_rows)

    def plane_copy(c, g):
        mine_at, there = xsend.at[c, part_of(g)], xrecv.at[chip, part_of(g)]
        return remote(mine_at, there, xs_sem.at[c, g], xr_sem.at[chip, g], on_chip(c))

    def plane_arrival(c, g):
        mine_at, here = xsend.at[c, part_of(g)], xrecv.at[c, part_of(g)]
        return remote(mine_at, here, xs_sem.at[c, g], xr_sem.at[c, g], on_chip(c))

    def plane_sq(c):
        return remote(xsq.at[chip], xsq.at[chip], xsqs_sem.at[c], xsqr_sem.at[chip], on_chip(c))

    def plane_sq_arrival(c):
        return remote(xsq.at[c], xsq.at[c], xsqs_sem.at[c], xsqr_sem.at[c], on_chip(c))

    def depth_copy(par, k, g):
        block = zbuf.at[par, z, part_of(g)]
        return remote(block, block, zs_sem.at[par, k, g], zr_sem.at[par, z, g], on_plane(k))

    def depth_arrival(par, k, g):
        block = zbuf.at[par, k, part_of(g)]
        return remote(block, block, zs_sem.at[par, k, g], zr_sem.at[par, k, g], on_plane(k))

    def depth_sq(par, k):
        return remote(zsq.at[par, z], zsq.at[par, z], zsqs_sem.at[par, k], zsqr_sem.at[par, z], on_plane(k))

    def depth_sq_arrival(par, k):
        return remote(zsq.at[par, k], zsq.at[par, k], zsqs_sem.at[par, k], zsqr_sem.at[par, k], on_plane(k))

    def last_sq(k, other):
        there = (1 - core) if other else core
        return remote(fsq.at[core, z], fsq.at[core, z], fsqs_sem.at[there, k], fsqr_sem.at[core, z], on_plane(k, other))

    def last_sq_arrival(h, k):
        return remote(fsq.at[h, k], fsq.at[h, k], fsqs_sem.at[h, k], fsqr_sem.at[h, k], partner)

    def piece(c, g):
        return q.at[part_of(g), pl.ds(pl.multiple_of(c * LANES, LANES), LANES)]

    def gather_copy(c, g):
        return remote(piece(chip, g), piece(chip, g), gs_sem.at[c, g], gr_sem.at[chip, g], on_chip(c))

    def gather_arrival(c, g):
        return remote(piece(c, g), piece(c, g), gs_sem.at[c, g], gr_sem.at[c, g], on_chip(c))

    def keep_squares():
        square = pref[...] * pref[...]
        blank = jnp.zeros_like(square)
        square = jnp.concatenate(
            [jnp.where(core == 0, square, blank), jnp.where(core == 0, blank, square)], axis=0
        )
        high, low = halves(square)
        total = dot_nt(ones, high) + dot_nt(ones, low)
        csq[...] = total[0:1]

    def squares_plane():
        xsq[chip] = csq[...]
        for c in plane_chips:
            plane_sq(c).start()

    def squares_of_plane():
        for c in plane_chips:
            plane_sq_arrival(c).wait_recv()
        total = xsq[0]
        for c in range(1, CHIPS):
            total = total + xsq[c]
        return total

    def keep_norm(total):
        spread = jnp.transpose(jnp.broadcast_to(total, (columns, columns)))
        ucol[...] = jnp.sqrt(spread + FLOOR_SQ)

    def send_group(value, dy):
        line = row_at(dy) * SIDE
        for s in range(SIDE):
            block = value[:, s * LANES : (s + 1) * LANES]
            xsend[line + s] = block.astype(jnp.bfloat16)
            if dy == 0:
                ownrow[s] = block
        for dx in SEND_COLS:
            if dy or dx:
                plane_copy(chip_at(dy, dx), 0).start()

    raw[...] = jnp.zeros_like(raw)
    vinv[...] = jnp.zeros_like(vinv)
    state[...] = jnp.zeros_like(state)
    scalars[...] = jnp.zeros_like(scalars)
    load_count.wait()
    shown = (lax.broadcasted_iota(jnp.int32, (1, rows), 1) < count[0]).astype(jnp.float32)
    live[0] = shown
    load_b.wait()
    first_residue = shown * jnp.transpose(b[...].astype(jnp.float32))
    p0[pl.ds(0, columns)] = first_residue.astype(jnp.bfloat16)
    load_a.wait()
    load_n.start()

    start_residue = p0[pl.ds(0, columns)]
    for j in range(width // TILE):
        lanes = slice(j * TILE, (j + 1) * TILE)
        product = dot(start_residue, a[pl.ds(0, rows), lanes])
        part[:, lanes] = product
        partb[:, lanes] = product.astype(jnp.bfloat16)
    pl.semaphore_wait(barrier, len(partners))
    for dy in SEND_ROWS:
        core_copy(dy).start()
    residue_copy.start()
    live_copy.start()
    a_copy.start()

    mine = pl.ds(pl.multiple_of(lax.rem(z, per_core) * own_cols, own_cols), own_cols)
    spread = width // LANES

    def recur(first):
        u_own = ucol[pl.ds(pl.multiple_of(core * half, half) + lax.rem(z, per_core) * own_cols, own_cols)]
        v_own = vcol[mine]
        rho, phi, start = (scalars[core, pl.ds(k * own_cols, own_cols)] for k in range(3))
        search = state[core, pl.ds(own_cols, own_cols)]
        radius = jnp.sqrt(rho * rho + u_own * u_own)
        cosine = rho / radius
        sine = u_own / radius
        state[core, pl.ds(0, own_cols)] = (
            state[core, pl.ds(0, own_cols)] + wide(cosine * phi / radius, spread) * search
        )
        state[core, pl.ds(own_cols, own_cols)] = raw[mine] * wide(vinv[mine], spread) - wide(sine * v_own / radius, spread) * search
        scalars[core, pl.ds(0, own_cols)] = jnp.where(first, v_own, -cosine * v_own)
        scalars[core, pl.ds(own_cols, own_cols)] = jnp.where(first, u_own, sine * phi)
        scalars[core, pl.ds(2 * own_cols, own_cols)] = jnp.where(first, u_own, start)

    def group_arrival(dy):
        for dx in SEND_COLS:
            if dy or dx:
                for g in range(PARTS):
                    gather_arrival(chip_at(dy, dx), g).wait_recv()

    def folded(value):
        total = value[:, :LANES] * value[:, :LANES]
        for k in range(1, value.shape[1] // LANES):
            block = value[:, k * LANES : (k + 1) * LANES]
            total = total + block * block
        return total

    def multiply(first):
        lines = pl.ds(first, rows)

        def step(k, c):
            here = pl.ds(pl.multiple_of(k * 2 * TILE, 2 * TILE), 2 * TILE)
            bm[lines, here] = dot(a[lines], n[:, here]).astype(jnp.bfloat16)
            return c

        lax.fori_loop(0, width // (2 * TILE), step, 0)

    def flip():
        lines = lax.broadcasted_iota(jnp.int32, (TILE, TILE), 0)
        same = (lines == lax.broadcasted_iota(jnp.int32, (TILE, TILE), 1)).astype(jnp.bfloat16)

        def step(k, c):
            here = pl.ds(pl.multiple_of(k * TILE, TILE), TILE)
            for j in range(width // TILE):
                lanes = slice(j * TILE, (j + 1) * TILE)
                bt[lanes, here] = dot_nt(same, bm[here, lanes]).astype(jnp.bfloat16)
            return c

        lax.fori_loop(0, both // TILE, step, 0)

    def turn(i, carry):
        par = lax.rem(i, 2)

        @pl.when(i == 0)
        def _():
            for dy in SEND_ROWS:
                core_copy(dy).wait_recv()
                lanes = pl.ds(pl.multiple_of(row_at(dy) * GROUP, GROUP), GROUP)
                send_group(part[ours, lanes] + crecv[:, lanes].astype(jnp.float32), dy)
            residue_copy.wait_recv()
            pref[...] = jnp.concatenate([p0[ours], p0[pl.ds(columns, half)]], axis=1).astype(jnp.float32)

        @pl.when(i > 0)
        def _():
            residue = pb[...]
            for dy in SEND_ROWS:
                lanes = pl.ds(pl.multiple_of(row_at(dy) * GROUP, GROUP), GROUP)
                send_group(dot(residue, bm[:, lanes]), dy)

        for g in range(1, PARTS):
            for c in plane_chips:
                plane_copy(c, g).start()
        keep_squares()
        squares_plane()

        @pl.when(i > 0)
        def _():
            recur(i == 1)

        @pl.when(i == 0)
        def _():
            load_n.wait()
            multiply(0)

        for g in range(PARTS):
            own = ownrow[x, part_of(g)]
            for c in plane_chips:
                plane_arrival(c, g).wait_recv()
                own = own + xrecv[c, part_of(g)].astype(jnp.float32)
            zbuf[par, z, part_of(g)] = own.astype(jnp.bfloat16)
            for k in other_planes:
                depth_copy(par, k, g).start()
        zsq[par, z] = squares_of_plane()
        for k in other_planes:
            depth_sq(par, k).start()

        @pl.when(i == 0)
        def _():
            a_copy.wait_recv()
            live_copy.wait_recv()
            multiply(rows)

        for g in range(PARTS):
            for k in other_planes:
                depth_arrival(par, k, g).wait_recv()
            total = zbuf[par, 0, part_of(g)].astype(jnp.float32)
            for k in range(1, planes):
                total = total + zbuf[par, k, part_of(g)].astype(jnp.float32)
            q[part_of(g), pl.ds(pl.multiple_of(chip * LANES, LANES), LANES)] = total.astype(jnp.bfloat16)

            for c in plane_chips:
                gather_copy(c, g).start()
        for k in other_planes:
            depth_sq_arrival(par, k).wait_recv()
        total = zsq[par, 0]
        for k in range(1, planes):
            total = total + zsq[par, k]
        keep_norm(total)
        u = ucol[ours]
        shrink = 1.0 / u
        for c in plane_chips:
            for g in range(PARTS):
                plane_copy(c, g).wait_send()
            plane_sq(c).wait_send()
        for k in other_planes:
            for g in range(PARTS):
                depth_copy(par, k, g).wait_send()
            depth_sq(par, k).wait_send()

        @pl.when(i == 0)
        def _():
            flip()
            squares = jnp.zeros((half, LANES), jnp.float32)
            for taken, dy in enumerate(TAKE_ROWS):
                group_arrival(dy)
                here = group(dy)
                value = q[:, here]
                for j in range(width // TILE):
                    lanes = slice(j * TILE, (j + 1) * TILE)
                    product = dot(value, n[here, lanes])
                    if taken:
                        product = raw[:, lanes] + product
                    if taken == SIDE - 1:
                        product = product * wide(shrink, TILE // LANES)
                    raw[:, lanes] = product
                    if taken == SIDE - 1:
                        squares = squares + folded(product)
            sums[...] = squares
            image[...] = dot(raw[...].astype(jnp.bfloat16), bt[...])

        @pl.when(i > 0)
        def _():
            back = wide(u * vinv[...], SIDE)
            squares = jnp.zeros((half, LANES), jnp.float32)
            for taken, dy in enumerate(TAKE_ROWS):
                group_arrival(dy)
                here = group(dy)
                value = wide(shrink, SIDE) * q[:, here].astype(jnp.float32) - back * raw[:, here]
                raw[:, here] = value
                product = dot(value.astype(jnp.bfloat16), bt[here, :])
                image[...] = image[...] + product if taken else product
                squares = squares + folded(value)
            sums[...] = squares

        v = jnp.sqrt(jnp.sum(sums[...], axis=1, keepdims=True) + FLOOR_SQ)
        v = jnp.broadcast_to(v, (half, LANES))
        inverse = 1.0 / v
        vcol[...] = v
        vinv[...] = inverse

        scale, back = wide(inverse, rows // LANES), wide(v / u, rows // LANES)
        for h in range(2):
            lanes = slice(h * rows, (h + 1) * rows)
            residue = live[h] * (scale * image[:, lanes] - back * pref[:, lanes])
            pref[:, lanes] = residue
            pb[:, lanes] = residue.astype(jnp.bfloat16)

        for c in plane_chips:
            for g in range(PARTS):
                gather_copy(c, g).wait_send()
        return carry

    lax.fori_loop(0, ITERS, turn, 0)

    keep_squares()
    squares_plane()
    recur(ITERS == 1)
    fsq[core, z] = squares_of_plane()
    last_core = remote(fsq.at[core, z], fsq.at[core, z], fsqs_sem.at[1 - core, z], fsqr_sem.at[core, z], partner)
    for k in other_planes:
        last_sq(k, False).start()
        last_sq(k, True).start()
    last_core.start()
    state_copy.start()
    scalars_copy.start()

    holder = lax.div(z, per_core)
    state_arrival.wait_recv()
    scalars_arrival.wait_recv()
    high, low = halves(state[holder])
    stacked = jnp.concatenate([high, low], axis=0)
    for j in range(width // TILE):
        lanes = slice(j * TILE, (j + 1) * TILE)
        product = dot_nt(stacked, n[lanes, :])
        raw[pl.ds(0, 2 * own_cols), lanes] = product[: 2 * own_cols] + product[2 * own_cols :]

    last_sq_arrival(1 - core, z).wait_recv()
    for k in other_planes:
        last_sq_arrival(0, k).wait_recv()
        last_sq_arrival(1, k).wait_recv()
    total = fsq[0, 0]
    for h in range(2):
        for k in range(planes):
            if h or k:
                total = total + fsq[h, k]
    keep_norm(total)
    u_own = ucol[pl.ds(pl.multiple_of(z * own_cols, own_cols), own_cols)]
    rho, phi, start = (scalars[holder, pl.ds(k * own_cols, own_cols)] for k in range(3))
    radius = jnp.sqrt(rho * rho + u_own * u_own)
    cosine = rho / radius
    sine = u_own / radius
    step = wide(cosine * phi / radius, spread)
    coef_ref[...] = state[holder, pl.ds(0, own_cols)] + step * state[holder, pl.ds(own_cols, own_cols)]
    sol_ref[...] = raw[pl.ds(0, own_cols)] + step * raw[pl.ds(own_cols, own_cols)]
    ratio_ref[...] = sine * phi / start

    for dy in SEND_ROWS:
        core_copy(dy).wait_send()
    for copy in (residue_copy, live_copy, a_copy, state_copy, scalars_copy, last_core):
        copy.wait_send()
    for c in plane_chips:
        plane_sq(c).wait_send()
    for k in other_planes:
        last_sq(k, False).wait_send()
        last_sq(k, True).wait_send()


def finish(sol_in, coef_in, ratio_in, sol_ref, coef_ref, ratio_ref):
    sol_ref[...] = sol_in[...]
    coef_ref[...] = coef_in[...]
    ratio = ratio_in[...]
    square = jnp.concatenate([ratio] * (LANES // ratio.shape[0]), axis=0)
    ratio_ref[...] = jnp.transpose(square)[0:1, : ratio.shape[0]]


def shards(planes, matrix, right_side, precond, row_counts):
    rows, width = matrix.shape
    columns = right_side.shape[1]
    own_cols = columns // planes
    half = columns // 2
    vmem, dma = pltpu.VMEM, pltpu.SemaphoreType.DMA
    bf16, f32 = jnp.bfloat16, jnp.float32
    solution, coeffs, ratio = pl.pallas_call(
        functools.partial(kernel, planes),
        out_shape=(
            jax.ShapeDtypeStruct((own_cols, width), f32),
            jax.ShapeDtypeStruct((own_cols, width), f32),
            jax.ShapeDtypeStruct((own_cols, LANES), f32),
        ),
        in_specs=[pl.BlockSpec(memory_space=pl.ANY)] * 4,
        out_specs=(pl.BlockSpec(memory_space=vmem),) * 3,
        scratch_shapes=[
            pltpu.SMEM((1,), jnp.int32),
            vmem((2 * rows, width), bf16),
            vmem((rows, columns), bf16),
            vmem((width, width), bf16),
            vmem((2 * rows, width), bf16),
            vmem((width, 2 * rows), bf16),
            vmem((half, width), f32),
            vmem((half, 2 * rows), f32),
            vmem((half, 2 * rows), f32),
            vmem((half, 2 * rows), bf16),
            vmem((columns + half, rows), bf16),
            vmem((half, width), bf16),
            vmem((columns, width), f32),
            vmem((columns, width), bf16),
            vmem((half, width), bf16),
            vmem((CHIPS, half, LANES), bf16),
            vmem((CHIPS, half, LANES), bf16),
            vmem((SIDE, half, LANES), f32),
            vmem((2, planes, half, LANES), bf16),
            vmem((2, 1, rows), f32),
            vmem((1, columns), f32),
            vmem((CHIPS, 1, columns), f32),
            vmem((2, planes, 1, columns), f32),
            vmem((2, planes, 1, columns), f32),
            vmem((2, 2 * own_cols, width), f32),
            vmem((2, 3 * own_cols, LANES), f32),
            vmem((columns, LANES), f32),
            vmem((half, LANES), f32),
            vmem((half, LANES), f32),
            vmem((half, LANES), f32),
            dma((4,)),
            dma((SIDE,)), dma((SIDE,)), dma, dma, dma, dma, dma, dma,
            dma((CHIPS, PARTS)), dma((CHIPS, PARTS)),
            dma((2, planes, PARTS)), dma((2, planes, PARTS)),
            dma((CHIPS, PARTS)), dma((CHIPS, PARTS)),
            dma((CHIPS,)), dma((CHIPS,)),
            dma((2, planes)), dma((2, planes)),
            dma((2, planes)), dma((2, planes)),
            dma, dma, dma, dma,
        ],
        compiler_params=pltpu.CompilerParams(
            collective_id=0, has_side_effects=True, vmem_limit_bytes=60 * 1024 * 1024
        ),
    )(row_counts, matrix, right_side, precond)
    solution, coeffs, ratio = pl.pallas_call(
        finish,
        out_shape=(
            jax.ShapeDtypeStruct((own_cols, width), f32),
            jax.ShapeDtypeStruct((own_cols, width), f32),
            jax.ShapeDtypeStruct((1, own_cols), f32),
        ),
    )(solution, coeffs, ratio)
    return solution.T, coeffs.T, ratio[0]


def solution(mesh):
    return jax.shard_map(
        functools.partial(shards, mesh.shape["grp"]),
        mesh=mesh,
        in_specs=(P(("rows", "grp"), None), P(("rows", "grp"), None), P(), P(("rows", "grp"))),
        out_specs=(P(None, "grp"), P(None, "grp"), P("grp")),
        check_vma=False,
    )
```
